256 devices in a mesh: grp: 2 (over z), seq: 128 (over x, y, core).
Axes of the slice: x: 8, y: 8, z: 2, core: 2. Of those that a mesh axis runs over, the one named last changes fastest.
The devices are a block of a 8x8x16 slice.
Arguments:
- queries: bfloat16 [65536, 32, 128], P(('grp', 'seq')), parts along dimension 0, may hold values from -45 to 45
- keys: bfloat16 [65536, 8, 128], P(('grp', 'seq')), parts along dimension 0, may hold values from -6 to 6
- values: bfloat16 [65536, 8, 128], P(('grp', 'seq')), parts along dimension 0, may hold values from -6 to 6
- global_ids: int32 [8], P('grp'), parts along dimension 0, may hold values from 0 to 255, as said below
- doc_lengths: int32 [32], P('grp'), parts along dimension 0, may hold values from 1 to 8192, 32768 in all
Outputs:
- attended: bfloat16 [65536, 32, 128], P(('grp', 'seq')), parts along dimension 0
The draws below stay inside these ranges and needn't reach their ends.
There are 2 independent parts, one for each index of `grp`. The reference program is written for one: setup_inputs(seed, part) draws one part's arguments, and reference() takes and returns one part's arrays. A program takes and returns all parts, laid end to end along the dimension named above; each array names one. Nothing has to cross between parts.
Inputs may be any that keep to these rules, and one draw needn't show every extreme that they name: `global_ids`: 4 distinct block numbers.
All inputs are finite; a program needn't handle non-finite values.
Results may differ from the reference program's by a relative error of at most 0.0065.
Values may be sent and summed in bfloat16 or wider, within the bound.
No kernel may reach another device: no remote copies, remote signals or barrier semaphores. Data moves between devices by JAX's collectives and lax.ppermute only.
A program may use at most 64 MiB of HBM per device.

```python
import math
import jax
import jax.numpy as jnp
import numpy as np
from jax import lax

HEADS = 32
KV_HEADS = 8
HEAD_DIM = 128
BLK = 128
WIN = 3
GLOBAL_BLOCKS = 4
NDOC = 16
TOKENS = 32768
NBLK = 256
MOST_DOC = 8192


def key_field(key):
    return jnp.clip(jax.random.normal(jax.random.fold_in(key, 11), (TOKENS, KV_HEADS, HEAD_DIM), jnp.float32), -6.0, 6.0)


def draw_keys(key, part):
    field = key_field(key)
    return field.astype(jnp.bfloat16)


def draw_queries(key, part):
    drawn = jnp.clip(jax.random.normal(jax.random.fold_in(key, 19), (TOKENS, HEADS, HEAD_DIM), jnp.float32), -6.0, 6.0)
    return drawn.astype(jnp.bfloat16)


def draw_global_ids(key, part):
    shuffled = jax.random.permutation(jax.random.fold_in(key, 5), NBLK)
    return shuffled[:GLOBAL_BLOCKS].astype(jnp.int32)


def steps_of(own_key, shape, pieces, smallest, largest):
    def one(axis_at, blocks):
        draws = jax.random.uniform(jax.random.fold_in(jax.random.fold_in(own_key, 6), axis_at), (blocks,), jnp.float32, smallest / len(pieces), largest / len(pieces))
        return jnp.repeat(jnp.exp(draws), shape[axis_at] // blocks).reshape((-1,) + (1,) * (len(shape) - axis_at - 1))

    loudness = one(*pieces[0])
    for cut in pieces[1:]:
        loudness = loudness * one(*cut)
    return loudness


def profile(amount, total, limit, skew):
    portions = [(1 << 20) // math.isqrt(grade ** skew) + 1 for grade in range(2, amount + 1)]
    spare, counts = total - limit - (amount - 1), [1] * (amount - 1)
    while spare > 0:
        free = [i for i in range(amount - 1) if counts[i] < limit]
        whole, budget = sum([portions[i] for i in free]), spare
        for i in free:
            addition = min(limit - counts[i], max(1, budget * portions[i] // whole), spare)
            counts[i] = counts[i] + addition
            spare = spare - addition
    return np.array([limit] + counts)


def ragged_sizes(rng, count, total, bound, slope):
    if count == 2:
        one = jax.random.randint(rng, (), max(1, total - bound), min(bound, total - 1) + 1)
        return jnp.stack([one, total - one])
    lengths = jnp.asarray(profile(count, total, bound, slope), jnp.int32)
    couples = (count - 1) // 2
    donor, sink = lengths[1:1 + 2 * couples:2], lengths[2:2 + 2 * couples:2]
    slack = jnp.minimum(donor - 1, bound - sink)
    passed = jax.random.randint(jax.random.fold_in(rng, 1), (couples,), 0, 1 << 20) % (slack + 1)
    lengths = lengths.at[1:1 + 2 * couples:2].set(donor - passed).at[2:2 + 2 * couples:2].set(sink + passed)
    return lengths[jax.random.permutation(jax.random.fold_in(rng, 2), count)]


def bell_draw(stream_key, dims, width, most, cuts=(), held_as=jnp.bfloat16):
    values = width * jax.random.normal(stream_key, dims, jnp.float32)
    if cuts:
        values = values * steps_of(stream_key, dims, cuts, -0.22, 0.18)
    return jnp.clip(values, -most, most).astype(held_as)


def setup_inputs(seed: int = 0, part: int = 0) -> dict:
    key_list = jax.random.split(jax.random.key(seed), 6)
    part_splits = jax.random.split(jax.random.fold_in(key_list[5], part), 6)
    queries = draw_queries(jax.random.fold_in(jax.random.fold_in(key_list[5], part), 71), part)
    keys = draw_keys(jax.random.fold_in(jax.random.fold_in(key_list[5], part), 71), part)
    values = bell_draw(part_splits[2], (TOKENS, KV_HEADS, HEAD_DIM), 1.0, 6.0, ((0, 128),))
    global_ids = draw_global_ids(jax.random.fold_in(jax.random.fold_in(key_list[5], part), 71), part)
    doc_lengths = ragged_sizes(part_splits[4], NDOC, TOKENS, MOST_DOC, 2).astype(jnp.int32)
    return {"queries": queries, "keys": keys, "values": values, "global_ids": global_ids, "doc_lengths": doc_lengths}


masked_score = -1e+30

def doc_index(positions, doc_ends):
    return lax.optimization_barrier(jnp.sum((positions[:, None] >= doc_ends[None, :]).astype(jnp.int32), axis=1))

def reference(queries, keys, values, global_ids, doc_lengths):
    group_size = HEADS // KV_HEADS
    score_scale = 1.0 / math.sqrt(HEAD_DIM)
    doc_ends = jnp.cumsum(doc_lengths).astype(jnp.int32)
    offsets = jnp.arange(BLK, dtype=jnp.int32)
    padding = jnp.zeros(((WIN - 1) * BLK, KV_HEADS, HEAD_DIM), keys.dtype)
    key_pad = jnp.concatenate([padding, keys], axis=0)
    val_pad = jnp.concatenate([padding, values], axis=0)
    glob_keys = keys.reshape(NBLK, BLK, KV_HEADS, HEAD_DIM)[global_ids].reshape(GLOBAL_BLOCKS * BLK, KV_HEADS, HEAD_DIM)
    glob_vals = values.reshape(NBLK, BLK, KV_HEADS, HEAD_DIM)[global_ids].reshape(GLOBAL_BLOCKS * BLK, KV_HEADS, HEAD_DIM)
    glob_block = jnp.repeat(global_ids, BLK).astype(jnp.int32)
    window_span = jnp.arange(WIN * BLK, dtype=jnp.int32)

    def one_block(block_id):
        first_row = (block_id * BLK).astype(jnp.int32)
        query_pos = first_row + offsets
        query_doc = doc_index(query_pos, doc_ends)
        query_rows = lax.dynamic_slice_in_dim(queries, first_row, BLK, 0).astype(jnp.float32)
        query_rows = query_rows.reshape(BLK, KV_HEADS, group_size, HEAD_DIM)
        win_keys = lax.dynamic_slice_in_dim(key_pad, first_row, WIN * BLK, 0)
        win_vals = lax.dynamic_slice_in_dim(val_pad, first_row, WIN * BLK, 0)
        win_pos = first_row - (WIN - 1) * BLK + window_span
        win_doc = doc_index(win_pos, doc_ends)
        win_ok = (win_pos[None, :] >= 0) & (win_pos[None, :] <= query_pos[:, None]) & (win_doc[None, :] == query_doc[:, None])
        block_gap = block_id - glob_block
        glob_line = jnp.logical_not((block_gap >= 0) & (block_gap < WIN))
        glob_ok = jnp.broadcast_to(glob_line[None, :], (BLK, GLOBAL_BLOCKS * BLK))
        allowed = jnp.concatenate([win_ok, glob_ok], axis=1)
        all_keys = jnp.concatenate([win_keys, glob_keys], axis=0).astype(jnp.float32)
        all_vals = jnp.concatenate([win_vals, glob_vals], axis=0).astype(jnp.float32)
        scores = jnp.einsum('qkgd,tkd->qkgt', query_rows, all_keys, precision=lax.Precision.HIGHEST) * score_scale
        mask_wide = allowed[:, None, None, :]
        scores = jnp.where(mask_wide, scores, masked_score)
        row_peak = lax.optimization_barrier(jnp.max(scores, axis=-1, keepdims=True))
        exp_terms = jnp.where(mask_wide, jnp.exp(scores - row_peak), 0.0)
        denominator = lax.optimization_barrier(jnp.sum(exp_terms, axis=-1))
        weights = lax.optimization_barrier(exp_terms.astype(jnp.bfloat16)).astype(jnp.float32)
        attended = jnp.einsum('qkgt,tkd->qkgd', weights, all_vals, precision=lax.Precision.HIGHEST) / denominator[..., None]
        return attended.astype(jnp.bfloat16).reshape(BLK, HEADS, HEAD_DIM)
    blocks = lax.map(one_block, jnp.arange(NBLK, dtype=jnp.int32))
    return blocks.reshape(TOKENS, HEADS, HEAD_DIM)
```

```python
import math

import jax
import jax.numpy as jnp
from jax import lax
from jax.experimental import pallas as pl
from jax.experimental.pallas import tpu as pltpu
from jax.sharding import PartitionSpec as P

BLK = 128
WIN = 3
masked_score = -1e30

HELD = (0, -3, 3, -1, -4, 2, 1, -2)


def ring_pairs(side, core0, core1):
    pairs = []
    for x in range(side):
        for y in range(side):
            for core, (dx, dy) in enumerate((core0, core1)):
                to = ((x + dx) % side) * side + (y + dy) % side
                pairs.append(((x * side + y) * 2 + core, to * 2 + core))
    return pairs


def along_scatter(shard, side, by):
    return lax.ppermute(shard, "seq", ring_pairs(side, (0, by), (by, 0)))


def across_scatter(shard, side, by):
    return lax.ppermute(shard, "seq", ring_pairs(side, (by, 0), (0, by)))


def pick(flag, one, other):
    return jnp.where(flag[:, None, None], one, other)


def gather_globals(keys, values, global_ids):
    devices = lax.axis_size("seq")
    side = math.isqrt(devices // 2)
    rank = lax.axis_index("seq")
    core, chip = rank % 2, rank // 2
    x, y = chip // side, chip % side
    heads, tok_rows, head_size = keys.shape
    slots = global_ids.shape[0]
    blocks_here = tok_rows // BLK
    blocks_chip = 2 * blocks_here
    owner = global_ids // blocks_chip
    owner_x, owner_y = owner // side, owner % side
    order = jnp.arange(slots)
    twins = (owner[:, None] == owner[None, :]) & (order[None, :] < order[:, None])
    turn = jnp.sum(twins.astype(jnp.int32), axis=1)
    is0 = core == 0
    cross_pos = jnp.where(is0, x, y)
    owner_ring = jnp.where(is0, owner_y, owner_x)
    owner_cross = jnp.where(is0, owner_x, owner_y)
    groups = [[(i * side + j) * 2 for j in range(side)] for i in range(side)]
    groups += [[(j * side + i) * 2 + 1 for j in range(side)] for i in range(side)]
    swap = [(i, i ^ 1) for i in range(devices)]

    def scatter(this_turn, held):
        mine = (owner == chip) & (turn == this_turn)
        local = jnp.sum(jnp.where(mine, global_ids - owner * blocks_chip, 0))
        local_core = local // blocks_here
        start = jnp.where(local_core == core, local % blocks_here, 0) * BLK
        key_part = lax.dynamic_slice_in_dim(keys, start, BLK, 1)
        val_part = lax.dynamic_slice_in_dim(values, start, BLK, 1)
        got = lax.ppermute(jnp.where(is0, val_part, key_part), "seq", swap)
        part = jnp.where(local_core == core, jnp.where(is0, key_part, val_part), got)
        parts = lax.all_to_all(part, "seq", 0, 0, axis_index_groups=groups, tiled=True)
        here = (owner_cross == cross_pos) & (turn == this_turn)
        return pick(here, parts[owner_ring], held)

    held = jnp.zeros((slots, BLK, head_size), keys.dtype)
    held = scatter(0, held)
    _, held = lax.while_loop(
        lambda carried: carried[0] <= jnp.max(turn),
        lambda carried: (carried[0] + 1, scatter(carried[0], carried[1])),
        (jnp.int32(1), held),
    )
    away = (owner_cross - cross_pos) % side
    down, up = across_scatter(held, side, 3), across_scatter(held, side, -3)
    held = pick(away == side - 3, down, pick(away == 3, up, held))
    down, up = across_scatter(held, side, 1), across_scatter(held, side, -1)
    from_down = (away == side - 1) | (away == side // 2) | (away == 2)
    from_up = (away == 1) | (away == side - 2)
    held = pick(from_down, down, pick(from_up, up, held))
    three = jnp.stack([held, along_scatter(held, side, 3), along_scatter(held, side, -3)])
    down, up = along_scatter(three, side, 1), along_scatter(three[:2], side, -1)
    own = jnp.concatenate([three, down, up]).reshape(heads, slots * BLK, head_size)
    other = lax.ppermute(own, "seq", swap)
    head = jnp.arange(heads, dtype=jnp.int32)
    place = [0] * side
    for at, offset in enumerate(HELD):
        place[offset % side] = at
    place = jnp.array(place, jnp.int32)
    key_at, val_at = place[(head - y) % side], place[(head - x) % side]
    return jnp.where(is0, own, other), jnp.where(is0, other, own), key_at, val_at


def over_keys(one, two):
    return lax.dot_general(one, two, (((0,), (0,)), ((), ())), preferred_element_type=jnp.float32)


def over_head(one, two):
    return lax.dot_general(one, two, (((1,), (1,)), ((), ())), preferred_element_type=jnp.float32)


def window_kernel(low_ref, q_ref, near_k, near_v, own_k, own_v, acc_ref, peak_ref, sum_ref, *, scale):
    group, tok_rows, head_size = q_ref.shape
    keys = jnp.concatenate([near_k[0], own_k[0]], axis=0)
    vals = jnp.concatenate([near_v[0], own_v[0]], axis=0)
    span = WIN * BLK
    rows = group * BLK
    for b in range(tok_rows // BLK):
        queries = q_ref[:, b * BLK : (b + 1) * BLK, :].reshape(rows, head_size)
        scores = over_head(keys[b * BLK : b * BLK + span], queries) * scale
        key_at = lax.broadcasted_iota(jnp.int32, (span, rows), 0) + b * BLK
        query_at = lax.broadcasted_iota(jnp.int32, (1, rows), 1) % BLK + (tok_rows + b * BLK)
        allowed = (key_at >= low_ref[b]) & (key_at <= query_at)
        scores = jnp.where(allowed, scores, masked_score)
        peak = jnp.max(scores, axis=0, keepdims=True)
        terms = jnp.exp2(scores - peak)
        sum_ref[0, b] = jnp.sum(terms, axis=0, keepdims=True)
        peak_ref[0, b] = peak
        acc_ref[0, b] = over_keys(vals[b * BLK : b * BLK + span], terms.astype(jnp.bfloat16))


def global_kernel(
    key_at, val_at, bias_ref, q_ref, gk_ref, gv_ref, acc_ref, peak_ref, sum_ref, out_ref, *, scale
):
    group, tok_rows, head_size = q_ref.shape
    rows = group * BLK
    slots = gk_ref.shape[1] // BLK
    for b in range(tok_rows // BLK):
        queries = q_ref[:, b * BLK : (b + 1) * BLK, :].reshape(rows, head_size)
        scores = over_head(gk_ref[0], queries) * scale
        before = peak_ref[0, b]
        peak = before
        parts = [scores[s * BLK : (s + 1) * BLK] for s in range(slots)]
        for s in range(slots):
            peak = jnp.maximum(peak, jnp.max(parts[s], axis=0, keepdims=True) + bias_ref[b, s])
        factor = jnp.exp2(before - peak)
        total = sum_ref[0, b] * factor
        terms = []
        for s in range(slots):
            term = jnp.exp2(parts[s] - (peak - bias_ref[b, s]))
            total = total + jnp.sum(term, axis=0, keepdims=True)
            terms.append(term.astype(jnp.bfloat16))
        acc = acc_ref[0, b] * factor + over_keys(gv_ref[0], jnp.concatenate(terms, axis=0))
        done = (acc / total).T.astype(out_ref.dtype)
        out_ref[:, b * BLK : (b + 1) * BLK, :] = done.reshape(group, BLK, head_size)


def per_device(queries, keys, values, global_ids, doc_lengths):
    tok_rows, heads_here, head_size = queries.shape
    kv_count = keys.shape[1]
    group = heads_here // kv_count
    blocks_here = tok_rows // BLK
    rows = group * BLK
    slots = global_ids.shape[0]
    scale = math.log2(math.e) / math.sqrt(head_size)
    rank = lax.axis_index("seq")
    first_pos = rank * tok_rows
    doc_ends = jnp.cumsum(doc_lengths)
    query_pos = first_pos + jnp.arange(tok_rows, dtype=jnp.int32)
    begun = doc_ends[None, :] <= query_pos[:, None]
    low = jnp.max(jnp.where(begun, doc_ends[None, :], 0), axis=1) - (first_pos - tok_rows)
    low = jnp.tile(low.reshape(blocks_here, 1, BLK), (1, 1, group))

    by_head = queries.transpose(1, 0, 2)
    key_heads, val_heads = keys.transpose(1, 0, 2), values.transpose(1, 0, 2)
    ring = [(i, i + 1) for i in range(lax.axis_size("seq") - 1)]
    near_k, near_v = lax.ppermute(key_heads, "seq", ring), lax.ppermute(val_heads, "seq", ring)

    per_head = pl.BlockSpec((1, tok_rows, head_size), lambda k, *_: (k, 0, 0))
    q_spec = pl.BlockSpec((group, tok_rows, head_size), lambda k, *_: (k, 0, 0))
    acc_spec = pl.BlockSpec((1, blocks_here, head_size, rows), lambda k, *_: (k, 0, 0, 0))
    row_spec = pl.BlockSpec((1, blocks_here, 1, rows), lambda k, *_: (k, 0, 0, 0))
    acc_shape = jax.ShapeDtypeStruct((kv_count, blocks_here, head_size, rows), jnp.float32)
    row_shape = jax.ShapeDtypeStruct((kv_count, blocks_here, 1, rows), jnp.float32)
    acc, peak, total = pl.pallas_call(
        lambda *refs: window_kernel(*refs, scale=scale),
        grid=(kv_count,),
        in_specs=[
            pl.BlockSpec((blocks_here, 1, rows), lambda k: (0, 0, 0)),
            q_spec, per_head, per_head, per_head, per_head,
        ],
        out_specs=[acc_spec, row_spec, row_spec],
        out_shape=[acc_shape, row_shape, row_shape],
        name="window_part",
    )(low, by_head, near_k, near_v, key_heads, val_heads)

    glob_k, glob_v, key_at, val_at = gather_globals(key_heads, val_heads, global_ids)
    block_gap = rank * blocks_here + jnp.arange(blocks_here, dtype=jnp.int32)[:, None] - global_ids
    bias = jnp.where((block_gap >= 0) & (block_gap < WIN), masked_score, 0.0).astype(jnp.float32)
    out = pl.pallas_call(
        lambda *refs: global_kernel(*refs, scale=scale),
        grid_spec=pltpu.PrefetchScalarGridSpec(
            num_scalar_prefetch=3,
            grid=(kv_count,),
            in_specs=[
                q_spec,
                pl.BlockSpec((1, slots * BLK, head_size), lambda k, ka, va, bias: (ka[k], 0, 0)),
                pl.BlockSpec((1, slots * BLK, head_size), lambda k, ka, va, bias: (va[k], 0, 0)),
                acc_spec, row_spec, row_spec,
            ],
            out_specs=q_spec,
        ),
        out_shape=jax.ShapeDtypeStruct((heads_here, tok_rows, head_size), jnp.bfloat16),
        name="global_part",
    )(key_at, val_at, bias, by_head, glob_k, glob_v, acc, peak, total)
    return out.transpose(1, 0, 2)


def solution(mesh):
    shard = P(("grp", "seq"), None, None)
    return jax.shard_map(
        per_device,
        mesh=mesh,
        in_specs=(shard, shard, shard, P("grp"), P("grp")),
        out_specs=shard,
        check_vma=False,
    )
```

```python
import math

import jax
import jax.numpy as jnp
from jax import lax
from jax.experimental import pallas as pl
from jax.experimental.pallas import tpu as pltpu
from jax.sharding import PartitionSpec as P

BLK = 128
WIN = 3
masked_score = -1e30

HELD = (0, -3, 3, -1, -4, 2, 1, -2)


def ring_pairs(side, core0, core1):
    pairs = []
    for x in range(side):
        for y in range(side):
            for core, (dx, dy) in enumerate((core0, core1)):
                to = ((x + dx) % side) * side + (y + dy) % side
                pairs.append(((x * side + y) * 2 + core, to * 2 + core))
    return pairs


def along_scatter(shard, side, by):
    return lax.ppermute(shard, "seq", ring_pairs(side, (0, by), (by, 0)))


def across_scatter(shard, side, by):
    return lax.ppermute(shard, "seq", ring_pairs(side, (by, 0), (0, by)))


def pick(flag, one, other):
    return jnp.where(flag[:, None, None], one, other)


def gather_globals(keys, values, global_ids, between):
    devices = lax.axis_size("seq")
    side = math.isqrt(devices // 2)
    rank = lax.axis_index("seq")
    core, chip = rank % 2, rank // 2
    x, y = chip // side, chip % side
    tok_rows, heads, head_size = keys.shape
    slots = global_ids.shape[0]
    blocks_here = tok_rows // BLK
    blocks_chip = 2 * blocks_here
    owner = global_ids // blocks_chip
    owner_x, owner_y = owner // side, owner % side
    order = jnp.arange(slots)
    twins = (owner[:, None] == owner[None, :]) & (order[None, :] < order[:, None])
    turn = jnp.sum(twins.astype(jnp.int32), axis=1)
    last_turn = jnp.max(turn)
    is0 = core == 0
    cross_pos = jnp.where(is0, x, y)
    owner_ring = jnp.where(is0, owner_y, owner_x)
    owner_cross = jnp.where(is0, owner_x, owner_y)
    groups = [[(i * side + j) * 2 for j in range(side)] for i in range(side)]
    groups += [[(j * side + i) * 2 + 1 for j in range(side)] for i in range(side)]
    swap = [(i, i ^ 1) for i in range(devices)]

    def scatter(this_turn, held):
        mine = (owner == chip) & (turn == this_turn)
        local = jnp.sum(jnp.where(mine, global_ids - owner * blocks_chip, 0))
        local_core = local // blocks_here
        start = jnp.where(local_core == core, local % blocks_here, 0) * BLK
        key_part = lax.dynamic_slice_in_dim(keys, start, BLK, 0)
        val_part = lax.dynamic_slice_in_dim(values, start, BLK, 0)
        got = lax.ppermute(jnp.where(is0, val_part, key_part), "seq", swap)
        part = jnp.where(local_core == core, jnp.where(is0, key_part, val_part), got)
        part = part.transpose(1, 0, 2)
        parts = lax.all_to_all(part, "seq", 0, 0, axis_index_groups=groups, tiled=True)
        here = (owner_cross == cross_pos) & (turn == this_turn)
        return pick(here, parts[owner_ring], held)

    held = jnp.zeros((slots, BLK, head_size), keys.dtype)
    held = scatter(0, held)
    _, held = lax.while_loop(
        lambda carried: carried[0] > 0,
        lambda carried: (carried[0] - 1, scatter(carried[0], carried[1])),
        (last_turn, held),
    )
    away = (owner_cross - cross_pos) % side
    before = held
    down, up = across_scatter(held, side, 3), across_scatter(held, side, -3)
    down, up = between[0](before, (down, up))
    held = pick(away == side - 3, down, pick(away == 3, up, held))
    down, up = across_scatter(held, side, 1), across_scatter(held, side, -1)
    from_down = (away == side - 1) | (away == side // 2) | (away == 2)
    from_up = (away == 1) | (away == side - 2)
    held = pick(from_down, down, pick(from_up, up, held))
    before = held
    down, up = along_scatter(held, side, 3), along_scatter(held, side, -3)
    down, up = between[1](before, (down, up))
    three = jnp.stack([held, down, up])
    down, up = along_scatter(three, side, 1), along_scatter(three[:2], side, -1)
    own = jnp.concatenate([three, down, up]).reshape(heads, slots * BLK, head_size)
    other = lax.ppermute(own, "seq", swap)
    return own, other


def over_keys(one, two):
    return lax.dot_general(one, two, (((0,), (0,)), ((), ())), preferred_element_type=jnp.float32)


def over_head(one, two):
    return lax.dot_general(one, two, (((1,), (1,)), ((), ())), preferred_element_type=jnp.float32)


def window_kernel(low_ref, q_ref, near_ref, own_ref, *refs, scale):
    acc_ref, peak_ref, sum_ref = refs[-3:]
    group, tok_rows, head_size = q_ref.shape
    keys = jnp.concatenate([near_ref[0, 0], own_ref[0, 0]], axis=0)
    vals = jnp.concatenate([near_ref[1, 0], own_ref[1, 0]], axis=0)
    span = WIN * BLK
    rows = group * BLK
    for b in range(tok_rows // BLK):
        queries = q_ref[:, b * BLK : (b + 1) * BLK, :].reshape(rows, head_size)
        scores = over_head(keys[b * BLK : b * BLK + span], queries) * scale
        key_at = lax.broadcasted_iota(jnp.int32, (span, rows), 0) + b * BLK
        query_at = lax.broadcasted_iota(jnp.int32, (1, rows), 1) % BLK + (tok_rows + b * BLK)
        allowed = (key_at >= low_ref[b]) & (key_at <= query_at)
        scores = jnp.where(allowed, scores, masked_score)
        peak = jnp.max(scores, axis=0, keepdims=True)
        terms = jnp.exp2(scores - peak)
        sum_ref[0, b] = jnp.sum(terms, axis=0, keepdims=True)
        peak_ref[0, b] = peak
        acc_ref[0, b] = over_keys(vals[b * BLK : b * BLK + span], terms.astype(jnp.bfloat16))


def global_kernel(
    place, rank_ref, ids, q_ref, own_ref, other_ref, acc_ref, peak_ref, sum_ref, out_ref, *, scale
):
    pair, blocks_here, head_size, rows = acc_ref.shape
    side = place.shape[0]
    group = rows // BLK
    slots = ids.shape[0]
    rank = rank_ref[0]
    chip = lax.div(rank, 2)
    x, y = lax.div(chip, side), lax.rem(chip, side)
    is0 = lax.rem(rank, 2) == 0
    first = pl.program_id(0) * pair
    gap_bias = []
    for b in range(blocks_here):
        gaps = [rank * blocks_here + b - ids[s] for s in range(slots)]
        gap_bias.append([jnp.where((g >= 0) & (g < WIN), masked_score, 0.0) for g in gaps])
    pairs = []
    for j in range(pair):
        key_at = place[lax.rem(first + j - y + side, side)]
        val_at = place[lax.rem(first + j - x + side, side)]
        pairs.append((
            jnp.where(is0, own_ref[key_at], other_ref[key_at]),
            jnp.where(is0, other_ref[val_at], own_ref[val_at]),
        ))
    for b in range(blocks_here):
        outs = []
        for j, (keys, vals) in enumerate(pairs):
            queries = q_ref[j * group : (j + 1) * group, b * BLK : (b + 1) * BLK, :]
            scores = over_head(keys, queries.reshape(rows, head_size)) * scale
            before = peak_ref[j, b]
            peak = before
            parts = [scores[s * BLK : (s + 1) * BLK] for s in range(slots)]
            for s in range(slots):
                top = jnp.max(parts[s], axis=0, keepdims=True)
                peak = jnp.maximum(peak, top + gap_bias[b][s])
            factor = jnp.exp2(before - peak)
            total = sum_ref[j, b] * factor
            terms = []
            for s in range(slots):
                term = jnp.exp2(parts[s] - (peak - gap_bias[b][s]))
                total = total + jnp.sum(term, axis=0, keepdims=True)
                terms.append(term.astype(jnp.bfloat16))
            acc = acc_ref[j, b] * factor + over_keys(vals, jnp.concatenate(terms, axis=0))
            outs.append((acc * (1.0 / total)).T.reshape(group, BLK, head_size))
        rows_out = jnp.transpose(jnp.concatenate(outs, axis=0), (1, 0, 2))
        out_ref[b * BLK : (b + 1) * BLK] = rows_out.astype(out_ref.dtype)


def per_device(queries, keys, values, global_ids, doc_lengths):
    tok_rows, heads_here, head_size = queries.shape
    kv_count = keys.shape[1]
    group = heads_here // kv_count
    blocks_here = tok_rows // BLK
    rows = group * BLK
    slots = global_ids.shape[0]
    scale = math.log2(math.e) / math.sqrt(head_size)
    rank = lax.axis_index("seq")
    devices = lax.axis_size("seq")
    side = math.isqrt(devices // 2)
    first_pos = rank * tok_rows
    doc_ends = jnp.cumsum(doc_lengths)
    query_pos = first_pos + jnp.arange(tok_rows, dtype=jnp.int32)
    begun = doc_ends[None, :] <= query_pos[:, None]
    low = jnp.max(jnp.where(begun, doc_ends[None, :], 0), axis=1) - (first_pos - tok_rows)
    low = jnp.tile(low.reshape(blocks_here, 1, BLK), (1, 1, group))

    by_head = queries.transpose(1, 0, 2)
    here = jnp.stack([keys, values]).transpose(0, 2, 1, 3)
    near = lax.ppermute(here, "seq", [(i, i + 1) for i in range(devices - 1)])

    parts = 2
    per_part = kv_count // parts
    acc_shape = jax.ShapeDtypeStruct((kv_count, blocks_here, head_size, rows), jnp.float32)
    row_shape = jax.ShapeDtypeStruct((kv_count, blocks_here, 1, rows), jnp.float32)
    work = kv_count * blocks_here * rows * BLK
    state = []

    def window_part(part, by_head):
        at = part * per_part
        two = pl.BlockSpec((2, 1, tok_rows, head_size), lambda k: (0, k + at, 0, 0))
        acc_spec = pl.BlockSpec((1, blocks_here, head_size, rows), lambda k: (k + at, 0, 0, 0))
        row_spec = pl.BlockSpec((1, blocks_here, 1, rows), lambda k: (k + at, 0, 0, 0))
        whole = [pl.BlockSpec(memory_space=pl.ANY)] * len(state)
        return pl.pallas_call(
            lambda *refs: window_kernel(*refs, scale=scale),
            grid=(per_part,),
            in_specs=[
                pl.BlockSpec((blocks_here, 1, rows), lambda k: (0, 0, 0)),
                pl.BlockSpec((group, tok_rows, head_size), lambda k: (k + at, 0, 0)),
                two, two, *whole,
            ],
            out_specs=[acc_spec, row_spec, row_spec],
            out_shape=[acc_shape, row_shape, row_shape],
            input_output_aliases={4 + i: i for i in range(len(state))},
            cost_estimate=pl.CostEstimate(
                flops=4 * work * WIN * head_size // parts,
                bytes_accessed=8 << 20,
                transcendentals=work * WIN // parts,
            ),
            compiler_params=pltpu.CompilerParams(vmem_limit_bytes=24 << 20),
            name=f"window_part_{part}",
        )(low, by_head, near, here, *state)

    def beside(part):
        def run(before, results):
            nonlocal state
            ready, _ = lax.optimization_barrier((by_head, before))
            state = window_part(part, ready)
            *results, acc, peak, total = lax.optimization_barrier((*results, *state))
            state = [acc, peak, total]
            return results

        return run

    own, other = gather_globals(keys, values, global_ids, [beside(part) for part in range(parts)])
    place = [0] * side
    for at, offset in enumerate(HELD):
        place[offset % side] = at
    pair = 2
    whole = pl.BlockSpec((kv_count, slots * BLK, head_size), lambda k, *_: (0, 0, 0))
    acc_spec = pl.BlockSpec((pair, blocks_here, head_size, rows), lambda k, *_: (k, 0, 0, 0))
    row_spec = pl.BlockSpec((pair, blocks_here, 1, rows), lambda k, *_: (k, 0, 0, 0))
    return pl.pallas_call(
        lambda *refs: global_kernel(*refs, scale=scale),
        grid_spec=pltpu.PrefetchScalarGridSpec(
            num_scalar_prefetch=3,
            grid=(kv_count // pair,),
            in_specs=[
                pl.BlockSpec((pair * group, tok_rows, head_size), lambda k, *_: (k, 0, 0)),
                whole, whole, acc_spec, row_spec, row_spec,
            ],
            out_specs=pl.BlockSpec((tok_rows, pair * group, head_size), lambda k, *_: (0, k, 0)),
        ),
        out_shape=jax.ShapeDtypeStruct((tok_rows, heads_here, head_size), jnp.bfloat16),
        compiler_params=pltpu.CompilerParams(vmem_limit_bytes=32 << 20),
        name="global_part",
    )(jnp.array(place, jnp.int32), rank.reshape(1), global_ids, by_head, own, other, *state)


def solution(mesh):
    shard = P(("grp", "seq"), None, None)
    return jax.shard_map(
        per_device,
        mesh=mesh,
        in_specs=(shard, shard, shard, P("grp"), P("grp")),
        out_specs=shard,
        check_vma=False,
    )
```

```python
import math

import jax
import jax.numpy as jnp
from jax import lax
from jax.experimental import pallas as pl
from jax.experimental.pallas import tpu as pltpu
from jax.sharding import PartitionSpec as P

BLK = 128
WIN = 3
masked_score = -1e30

HELD = (0, -3, 3, -1, -4, 2, 1, -2)


def ring_pairs(side, core0, core1):
    pairs = []
    for x in range(side):
        for y in range(side):
            for core, (dx, dy) in enumerate((core0, core1)):
                to = ((x + dx) % side) * side + (y + dy) % side
                pairs.append(((x * side + y) * 2 + core, to * 2 + core))
    return pairs


def along_scatter(shard, side, by):
    return lax.ppermute(shard, "seq", ring_pairs(side, (0, by), (by, 0)))


def across_scatter(shard, side, by):
    return lax.ppermute(shard, "seq", ring_pairs(side, (by, 0), (0, by)))


def pick(flag, one, other):
    return jnp.where(flag[:, None, None], one, other)


def gather_globals(keys, values, global_ids, prepare, between):
    devices = lax.axis_size("seq")
    side = math.isqrt(devices // 2)
    rank = lax.axis_index("seq")
    core, chip = rank % 2, rank // 2
    x, y = chip // side, chip % side
    tok_rows, heads, head_size = keys.shape
    slots = global_ids.shape[0]
    blocks_here = tok_rows // BLK
    blocks_chip = 2 * blocks_here
    owner = global_ids // blocks_chip
    owner_x, owner_y = owner // side, owner % side
    order = jnp.arange(slots)
    twins = (owner[:, None] == owner[None, :]) & (order[None, :] < order[:, None])
    turn = jnp.sum(twins.astype(jnp.int32), axis=1)
    last_turn = jnp.max(turn)
    is0 = core == 0
    cross_pos = jnp.where(is0, x, y)
    owner_ring = jnp.where(is0, owner_y, owner_x)
    owner_cross = jnp.where(is0, owner_x, owner_y)
    groups = [[(i * side + j) * 2 for j in range(side)] for i in range(side)]
    groups += [[(j * side + i) * 2 + 1 for j in range(side)] for i in range(side)]
    swap = [(i, i ^ 1) for i in range(devices)]

    mine = jnp.where(is0, keys, values)
    twin = lax.ppermute(jnp.where(is0, values, keys), "seq", swap)

    def scatter(this_turn, held, run):
        chosen = (owner == chip) & (turn == this_turn)
        local = jnp.sum(jnp.where(chosen, global_ids - owner * blocks_chip, 0))
        start = local % blocks_here * BLK
        part = jnp.where(
            local // blocks_here == core,
            lax.dynamic_slice_in_dim(mine, start, BLK, 0),
            lax.dynamic_slice_in_dim(twin, start, BLK, 0),
        ).transpose(1, 0, 2)
        parts = lax.all_to_all(part, "seq", 0, 0, axis_index_groups=groups, tiled=True)
        parts = run(part, parts)
        here = (owner_cross == cross_pos) & (turn == this_turn)
        return pick(here, parts[owner_ring], held)

    held = jnp.zeros((slots, BLK, head_size), keys.dtype)
    held = scatter(0, held, prepare)
    _, held = lax.while_loop(
        lambda carried: carried[0] > 0,
        lambda carried: (carried[0] - 1, scatter(*carried, lambda _, parts: parts)),
        (last_turn, held),
    )
    away = (owner_cross - cross_pos) % side
    before = held
    down, up = across_scatter(held, side, 3), across_scatter(held, side, -3)
    down, up = between[0](before, (down, up))
    held = pick(away == side - 3, down, pick(away == 3, up, held))
    down, up = across_scatter(held, side, 1), across_scatter(held, side, -1)
    from_down = (away == side - 1) | (away == side // 2) | (away == 2)
    from_up = (away == 1) | (away == side - 2)
    held = pick(from_down, down, pick(from_up, up, held))
    before = held
    down, up = along_scatter(held, side, 3), along_scatter(held, side, -3)
    down, up = between[1](before, (down, up))
    three = jnp.stack([held, down, up])
    down, up = along_scatter(three, side, 1), along_scatter(three[:2], side, -1)
    own = jnp.concatenate([three, down, up]).reshape(heads, slots * BLK, head_size)
    other = lax.ppermute(own, "seq", swap)
    return own, other


def over_keys(one, two):
    return lax.dot_general(one, two, (((0,), (0,)), ((), ())), preferred_element_type=jnp.float32)


def over_head(one, two):
    return lax.dot_general(one, two, (((1,), (1,)), ((), ())), preferred_element_type=jnp.float32)


def window_kernel(low_ref, q_ref, near_ref, own_ref, *refs, scale):
    acc_ref, peak_ref, sum_ref = refs[-3:]
    group, tok_rows, head_size = q_ref.shape
    keys = jnp.concatenate([near_ref[0, 0], own_ref[0, 0]], axis=0)
    vals = jnp.concatenate([near_ref[1, 0], own_ref[1, 0]], axis=0)
    span = WIN * BLK
    rows = group * BLK
    for b in range(tok_rows // BLK):
        queries = q_ref[:, b * BLK : (b + 1) * BLK, :].reshape(rows, head_size)
        scores = over_head(keys[b * BLK : b * BLK + span], queries) * scale
        key_at = lax.broadcasted_iota(jnp.int32, (span, rows), 0) + b * BLK
        query_at = lax.broadcasted_iota(jnp.int32, (1, rows), 1) % BLK + (tok_rows + b * BLK)
        allowed = (key_at >= low_ref[b]) & (key_at <= query_at)
        scores = jnp.where(allowed, scores, masked_score)
        peak = jnp.max(scores, axis=0, keepdims=True)
        terms = jnp.exp2(scores - peak)
        sum_ref[0, b] = jnp.sum(terms, axis=0, keepdims=True)
        peak_ref[0, b] = peak
        acc_ref[0, b] = over_keys(vals[b * BLK : b * BLK + span], terms.astype(jnp.bfloat16))


def global_kernel(
    place, rank_ref, ids, q_ref, own_ref, other_ref, acc_ref, peak_ref, sum_ref, out_ref, *, scale
):
    pair, blocks_here, head_size, rows = acc_ref.shape
    side = place.shape[0]
    group = rows // BLK
    slots = ids.shape[0]
    rank = rank_ref[0]
    chip = lax.div(rank, 2)
    x, y = lax.div(chip, side), lax.rem(chip, side)
    is0 = lax.rem(rank, 2) == 0
    first = pl.program_id(0) * pair
    gap_bias = []
    for b in range(blocks_here):
        gaps = [rank * blocks_here + b - ids[s] for s in range(slots)]
        gap_bias.append([jnp.where((g >= 0) & (g < WIN), masked_score, 0.0) for g in gaps])
    pairs = []
    for j in range(pair):
        key_at = place[lax.rem(first + j - y + side, side)]
        val_at = place[lax.rem(first + j - x + side, side)]
        pairs.append((
            jnp.where(is0, own_ref[key_at], other_ref[key_at]),
            jnp.where(is0, other_ref[val_at], own_ref[val_at]),
        ))
    for b in range(blocks_here):
        outs = []
        for j, (keys, vals) in enumerate(pairs):
            queries = q_ref[j * group : (j + 1) * group, b * BLK : (b + 1) * BLK, :]
            scores = over_head(keys, queries.reshape(rows, head_size)) * scale
            before = peak_ref[j, b]
            peak = before
            parts = [scores[s * BLK : (s + 1) * BLK] for s in range(slots)]
            for s in range(slots):
                top = jnp.max(parts[s], axis=0, keepdims=True)
                peak = jnp.maximum(peak, top + gap_bias[b][s])
            factor = jnp.exp2(before - peak)
            total = sum_ref[j, b] * factor
            terms = []
            for s in range(slots):
                term = jnp.exp2(parts[s] - (peak - gap_bias[b][s]))
                total = total + jnp.sum(term, axis=0, keepdims=True)
                terms.append(term.astype(jnp.bfloat16))
            acc = acc_ref[j, b] * factor + over_keys(vals, jnp.concatenate(terms, axis=0))
            outs.append((acc * (1.0 / total)).T.reshape(group, BLK, head_size))
        rows_out = jnp.transpose(jnp.concatenate(outs, axis=0), (1, 0, 2))
        out_ref[b * BLK : (b + 1) * BLK] = rows_out.astype(out_ref.dtype)


def per_device(queries, keys, values, global_ids, doc_lengths):
    tok_rows, heads_here, head_size = queries.shape
    kv_count = keys.shape[1]
    group = heads_here // kv_count
    blocks_here = tok_rows // BLK
    rows = group * BLK
    slots = global_ids.shape[0]
    scale = math.log2(math.e) / math.sqrt(head_size)
    rank = lax.axis_index("seq")
    devices = lax.axis_size("seq")
    side = math.isqrt(devices // 2)
    first_pos = rank * tok_rows
    doc_ends = jnp.cumsum(doc_lengths)
    query_pos = first_pos + jnp.arange(tok_rows, dtype=jnp.int32)
    parts = 2
    per_part = kv_count // parts
    acc_shape = jax.ShapeDtypeStruct((kv_count, blocks_here, head_size, rows), jnp.float32)
    row_shape = jax.ShapeDtypeStruct((kv_count, blocks_here, 1, rows), jnp.float32)
    work = kv_count * blocks_here * rows * BLK
    ready, state = [], []

    def prepare(before, result):
        *given, _ = lax.optimization_barrier((queries, keys, values, doc_ends, before))
        begun = given[3][None, :] <= query_pos[:, None]
        low = jnp.max(jnp.where(begun, given[3][None, :], 0), axis=1) - (first_pos - tok_rows)
        low = jnp.tile(low.reshape(blocks_here, 1, BLK), (1, 1, group))
        by_head = given[0].transpose(1, 0, 2)
        here = jnp.stack(given[1:3]).transpose(0, 2, 1, 3)
        near = lax.ppermute(here, "seq", [(i, i + 1) for i in range(devices - 1)])
        result, low, by_head, here = lax.optimization_barrier((result, low, by_head, here))
        ready.extend((low, by_head, near, here))
        return result

    def window_part(part, low, by_head, near, here):
        at = part * per_part
        two = pl.BlockSpec((2, 1, tok_rows, head_size), lambda k: (0, k + at, 0, 0))
        acc_spec = pl.BlockSpec((1, blocks_here, head_size, rows), lambda k: (k + at, 0, 0, 0))
        row_spec = pl.BlockSpec((1, blocks_here, 1, rows), lambda k: (k + at, 0, 0, 0))
        whole = [pl.BlockSpec(memory_space=pl.ANY)] * len(state)
        return pl.pallas_call(
            lambda *refs: window_kernel(*refs, scale=scale),
            grid=(per_part,),
            in_specs=[
                pl.BlockSpec((blocks_here, 1, rows), lambda k: (0, 0, 0)),
                pl.BlockSpec((group, tok_rows, head_size), lambda k: (k + at, 0, 0)),
                two, two, *whole,
            ],
            out_specs=[acc_spec, row_spec, row_spec],
            out_shape=[acc_shape, row_shape, row_shape],
            input_output_aliases={4 + i: i for i in range(len(state))},
            cost_estimate=pl.CostEstimate(
                flops=4 * work * WIN * head_size // parts,
                bytes_accessed=8 << 20,
                transcendentals=work * WIN // parts,
            ),
            compiler_params=pltpu.CompilerParams(vmem_limit_bytes=24 << 20),
            name=f"window_part_{part}",
        )(low, by_head, near, here, *state)

    def beside(part):
        def run(before, results):
            nonlocal state
            by_head, _ = lax.optimization_barrier((ready[1], before))
            state = window_part(part, ready[0], by_head, *ready[2:])
            *results, acc, peak, total = lax.optimization_barrier((*results, *state))
            state = [acc, peak, total]
            return results

        return run

    besides = [beside(part) for part in range(parts)]
    own, other = gather_globals(keys, values, global_ids, prepare, besides)
    place = [0] * side
    for at, offset in enumerate(HELD):
        place[offset % side] = at
    pair = 2
    whole = pl.BlockSpec((kv_count, slots * BLK, head_size), lambda k, *_: (0, 0, 0))
    acc_spec = pl.BlockSpec((pair, blocks_here, head_size, rows), lambda k, *_: (k, 0, 0, 0))
    row_spec = pl.BlockSpec((pair, blocks_here, 1, rows), lambda k, *_: (k, 0, 0, 0))
    return pl.pallas_call(
        lambda *refs: global_kernel(*refs, scale=scale),
        grid_spec=pltpu.PrefetchScalarGridSpec(
            num_scalar_prefetch=3,
            grid=(kv_count // pair,),
            in_specs=[
                pl.BlockSpec((pair * group, tok_rows, head_size), lambda k, *_: (k, 0, 0)),
                whole, whole, acc_spec, row_spec, row_spec,
            ],
            out_specs=pl.BlockSpec((tok_rows, pair * group, head_size), lambda k, *_: (0, k, 0)),
        ),
        out_shape=jax.ShapeDtypeStruct((tok_rows, heads_here, head_size), jnp.bfloat16),
        compiler_params=pltpu.CompilerParams(vmem_limit_bytes=32 << 20),
        name="global_part",
    )(jnp.array(place, jnp.int32), rank.reshape(1), global_ids, ready[1], own, other, *state)


def solution(mesh):
    shard = P(("grp", "seq"), None, None)
    return jax.shard_map(
        per_device,
        mesh=mesh,
        in_specs=(shard, shard, shard, P("grp"), P("grp")),
        out_specs=shard,
        check_vma=False,
    )
```

```python
import math

import jax
import jax.numpy as jnp
from jax import lax
from jax.experimental import pallas as pl
from jax.experimental.pallas import tpu as pltpu
from jax.sharding import PartitionSpec as P

BLK = 128
WIN = 3
masked_score = -1e30

HELD = (0, -3, 3, -1, -4, 2, 1, -2)

SEATS = 2


def ring_pairs(side, core0, core1):
    pairs = []
    for x in range(side):
        for y in range(side):
            for core, (dx, dy) in enumerate((core0, core1)):
                to = ((x + dx) % side) * side + (y + dy) % side
                pairs.append(((x * side + y) * 2 + core, to * 2 + core))
    return pairs


def along_scatter(shard, side, by):
    return lax.ppermute(shard, "seq", ring_pairs(side, (0, by), (by, 0)))


def across_scatter(shard, side, by):
    return lax.ppermute(shard, "seq", ring_pairs(side, (by, 0), (0, by)))


def pick(flag, one, other):
    return jnp.where(flag[:, None, None], one, other)


def owner_of(ids, slot, blocks_chip):
    return lax.div(ids[slot], blocks_chip)


def turn_of(ids, slot, blocks_chip):
    owner = owner_of(ids, slot, blocks_chip)
    return sum((owner_of(ids, s, blocks_chip) == owner).astype(jnp.int32) for s in range(slot))


def pick_kernel(rank_ref, ids, turn_ref, mine_ref, twin_ref, out_ref):
    blocks_here = mine_ref.shape[1] // BLK
    blocks_chip = 2 * blocks_here
    chip, core = lax.div(rank_ref[0], 2), lax.rem(rank_ref[0], 2)
    for lane in range(SEATS):
        count, local = jnp.int32(0), jnp.int32(0)
        for slot in range(ids.shape[0]):
            on_chip = owner_of(ids, slot, blocks_chip) == chip
            hit = on_chip & (count == turn_ref[0] * SEATS + lane)
            local = jnp.where(hit, lax.rem(ids[slot], blocks_chip), local)
            count = count + on_chip.astype(jnp.int32)
        from_mine = lax.div(local, blocks_here) == core
        start = pl.multiple_of(lax.rem(local, blocks_here) * BLK, BLK)
        to = pl.ds(lane * BLK, BLK)

        @pl.when(from_mine)
        def _():
            out_ref[:, to, :] = mine_ref[:, pl.ds(start, BLK), :]

        @pl.when(jnp.logical_not(from_mine))
        def _():
            out_ref[:, to, :] = twin_ref[:, pl.ds(start, BLK), :]


def seat_kernel(rank_ref, ids, turn_ref, parts_ref, *refs, blocks_chip, side):
    is0 = lax.rem(rank_ref[0], 2) == 0
    for slot in range(ids.shape[0]):
        owner = owner_of(ids, slot, blocks_chip)
        source = jnp.where(is0, lax.rem(owner, side), lax.div(owner, side))
        turn = turn_of(ids, slot, blocks_chip)
        start = pl.multiple_of(lax.rem(turn, SEATS) * BLK, BLK)
        part = parts_ref[source, pl.ds(start, BLK), :]
        if len(refs) > 1:
            part = jnp.where(lax.div(turn, SEATS) == turn_ref[0], part, refs[0][slot])
        refs[-1][slot] = part


def gather_globals(mine, twin, global_ids, besides):
    devices = lax.axis_size("seq")
    side = math.isqrt(devices // 2)
    rank = lax.axis_index("seq")
    core, chip = rank % 2, rank // 2
    x, y = chip // side, chip % side
    heads, tok_rows, head_size = mine.shape
    slots = global_ids.shape[0]
    blocks_chip = 2 * (tok_rows // BLK)
    owner = global_ids // blocks_chip
    order = jnp.arange(slots)
    twins = (owner[:, None] == owner[None, :]) & (order[None, :] < order[:, None])
    last_turn = jnp.max(jnp.sum(twins.astype(jnp.int32), axis=1)) // SEATS
    is0 = core == 0
    cross_pos = jnp.where(is0, x, y)
    owner_cross = jnp.where(is0, owner // side, owner % side)
    groups = [[(i * side + j) * 2 for j in range(side)] for i in range(side)]
    groups += [[(j * side + i) * 2 + 1 for j in range(side)] for i in range(side)]
    swap = [(i, i ^ 1) for i in range(devices)]
    scalars = [pl.BlockSpec(memory_space=pltpu.SMEM)] * 3
    vmem = pl.BlockSpec(memory_space=pltpu.VMEM)
    small = pltpu.CompilerParams(vmem_limit_bytes=16 << 20)

    def scatter(turn, held, run):
        spot = (rank.reshape(1), global_ids, turn.reshape(1))
        part = pl.pallas_call(
            pick_kernel,
            in_specs=[*scalars, vmem, vmem],
            out_specs=vmem,
            out_shape=jax.ShapeDtypeStruct((heads, SEATS * BLK, head_size), mine.dtype),
            compiler_params=small,
            name="pick",
        )(*spot, mine, twin)
        parts = lax.all_to_all(part, "seq", 0, 0, axis_index_groups=groups, tiled=True)
        parts = run(part, parts)
        return pl.pallas_call(
            lambda *refs: seat_kernel(*refs, blocks_chip=blocks_chip, side=side),
            in_specs=[*scalars, vmem, *[vmem] * len(held)],
            out_specs=vmem,
            out_shape=jax.ShapeDtypeStruct((slots, BLK, head_size), mine.dtype),
            compiler_params=small,
            name="seat",
        )(*spot, parts, *held)

    held = scatter(jnp.int32(0), [], besides[0])
    _, held = lax.while_loop(
        lambda carried: carried[0] > 0,
        lambda carried: (carried[0] - 1, scatter(carried[0], carried[1:], lambda _, parts: parts)),
        (last_turn, held),
    )
    away = (owner_cross - cross_pos) % side
    before = held
    down, up = across_scatter(held, side, 3), across_scatter(held, side, -3)
    down, up = besides[1](before, (down, up))
    held = pick(away == side - 3, down, pick(away == 3, up, held))
    before = held
    down, up = across_scatter(held, side, 1), across_scatter(held, side, -1)
    down, up = besides[2](before, (down, up))
    from_down = (away == side - 1) | (away == side // 2) | (away == 2)
    from_up = (away == 1) | (away == side - 2)
    held = pick(from_down, down, pick(from_up, up, held))
    before = held
    down, up = along_scatter(held, side, 3), along_scatter(held, side, -3)
    down, up = besides[3](before, (down, up))
    three = jnp.stack([held, down, up])
    before = three
    down, up = along_scatter(three, side, 1), along_scatter(three[:2], side, -1)
    down, up = besides[4](before, (down, up))
    own = jnp.concatenate([three, down, up]).reshape(heads, slots * BLK, head_size)
    other = lax.ppermute(own, "seq", swap)
    return own, other


def over_keys(one, two):
    return lax.dot_general(one, two, (((0,), (0,)), ((), ())), preferred_element_type=jnp.float32)


def over_head(one, two):
    return lax.dot_general(one, two, (((1,), (1,)), ((), ())), preferred_element_type=jnp.float32)


def window_kernel(rank_ref, low_ref, q_ref, near_mine, near_rest, mine, rest, *refs, scale):
    acc_ref, peak_ref, sum_ref = refs[-3:]
    group, tok_rows, head_size = q_ref.shape
    is0 = lax.rem(rank_ref[0], 2) == 0
    near_a, near_b, own_a, own_b = near_mine[0], near_rest[0], mine[0], rest[0]
    keys = [jnp.where(is0, near_b, near_a), jnp.where(is0, own_a, own_b)]
    vals = [jnp.where(is0, near_a, near_b), jnp.where(is0, own_b, own_a)]
    keys, vals = jnp.concatenate(keys, axis=0), jnp.concatenate(vals, axis=0)
    span = WIN * BLK
    rows = group * BLK
    for b in range(tok_rows // BLK):
        queries = q_ref[:, b * BLK : (b + 1) * BLK, :].reshape(rows, head_size)
        scores = over_head(keys[b * BLK : b * BLK + span], queries) * scale
        key_at = lax.broadcasted_iota(jnp.int32, (span, rows), 0) + b * BLK
        query_at = lax.broadcasted_iota(jnp.int32, (1, rows), 1) % BLK + (tok_rows + b * BLK)
        allowed = (key_at >= low_ref[b]) & (key_at <= query_at)
        scores = jnp.where(allowed, scores, masked_score)
        peak = jnp.max(scores, axis=0, keepdims=True)
        terms = jnp.exp2(scores - peak)
        sum_ref[0, b] = jnp.sum(terms, axis=0, keepdims=True)
        peak_ref[0, b] = peak
        acc_ref[0, b] = over_keys(vals[b * BLK : b * BLK + span], terms.astype(jnp.bfloat16))


def global_kernel(
    place, rank_ref, ids, q_ref, own_ref, other_ref, acc_ref, peak_ref, sum_ref, out_ref, *, scale
):
    pair, blocks_here, head_size, rows = acc_ref.shape
    side = place.shape[0]
    group = rows // BLK
    slots = ids.shape[0]
    rank = rank_ref[0]
    chip = lax.div(rank, 2)
    x, y = lax.div(chip, side), lax.rem(chip, side)
    is0 = lax.rem(rank, 2) == 0
    first = pl.program_id(0) * pair
    gap_bias = []
    for b in range(blocks_here):
        gaps = [rank * blocks_here + b - ids[s] for s in range(slots)]
        gap_bias.append([jnp.where((g >= 0) & (g < WIN), masked_score, 0.0) for g in gaps])
    pairs = []
    for j in range(pair):
        key_at = place[lax.rem(first + j - y + side, side)]
        val_at = place[lax.rem(first + j - x + side, side)]
        pairs.append((
            jnp.where(is0, own_ref[key_at], other_ref[key_at]),
            jnp.where(is0, other_ref[val_at], own_ref[val_at]),
        ))
    for b in range(blocks_here):
        outs = []
        for j, (keys, vals) in enumerate(pairs):
            queries = q_ref[j * group : (j + 1) * group, b * BLK : (b + 1) * BLK, :]
            scores = over_head(keys, queries.reshape(rows, head_size)) * scale
            before = peak_ref[j, b]
            peak = before
            parts = [scores[s * BLK : (s + 1) * BLK] for s in range(slots)]
            for s in range(slots):
                top = jnp.max(parts[s], axis=0, keepdims=True)
                peak = jnp.maximum(peak, top + gap_bias[b][s])
            factor = jnp.exp2(before - peak)
            total = sum_ref[j, b] * factor
            terms = []
            for s in range(slots):
                term = jnp.exp2(parts[s] - (peak - gap_bias[b][s]))
                total = total + jnp.sum(term, axis=0, keepdims=True)
                terms.append(term.astype(jnp.bfloat16))
            acc = acc_ref[j, b] * factor + over_keys(vals, jnp.concatenate(terms, axis=0))
            outs.append((acc * (1.0 / total)).T.reshape(group, BLK, head_size))
        rows_out = jnp.transpose(jnp.concatenate(outs, axis=0), (1, 0, 2))
        out_ref[b * BLK : (b + 1) * BLK] = rows_out.astype(out_ref.dtype)


def per_device(queries, keys, values, global_ids, doc_lengths):
    tok_rows, heads_here, head_size = queries.shape
    kv_count = keys.shape[1]
    group = heads_here // kv_count
    blocks_here = tok_rows // BLK
    rows = group * BLK
    slots = global_ids.shape[0]
    scale = math.log2(math.e) / math.sqrt(head_size)
    rank = lax.axis_index("seq")
    devices = lax.axis_size("seq")
    side = math.isqrt(devices // 2)
    first_pos = rank * tok_rows
    doc_ends = jnp.cumsum(doc_lengths)
    query_pos = first_pos + jnp.arange(tok_rows, dtype=jnp.int32)
    is0 = rank % 2 == 0
    mine = jnp.where(is0, keys, values).transpose(1, 0, 2)
    rest = jnp.where(is0, values, keys).transpose(1, 0, 2)
    twin = lax.ppermute(rest, "seq", [(i, i ^ 1) for i in range(devices)])

    acc_shape = jax.ShapeDtypeStruct((kv_count, blocks_here, head_size, rows), jnp.float32)
    row_shape = jax.ShapeDtypeStruct((kv_count, blocks_here, 1, rows), jnp.float32)
    work = blocks_here * rows * BLK * WIN
    ring = [(i, i + 1) for i in range(devices - 1)]
    ready, state = {}, []

    def send_near(before, result):
        mine_now, rest_now, ends, _ = lax.optimization_barrier((mine, rest, doc_ends, before))
        begun = ends[None, :] <= query_pos[:, None]
        low = jnp.max(jnp.where(begun, ends[None, :], 0), axis=1) - (first_pos - tok_rows)
        low = jnp.tile(low.reshape(blocks_here, 1, BLK), (1, 1, group))
        near = [lax.ppermute(part, "seq", ring) for part in (mine_now, rest_now)]
        result, low = lax.optimization_barrier((result, low))
        ready.update(low=low, near=near)
        return result

    def lay_queries(before, results):
        given, _ = lax.optimization_barrier((queries, before))
        *results, by_head = lax.optimization_barrier((*results, given.transpose(1, 0, 2)))
        ready.update(by_head=by_head)
        return results

    def window_part(first, count, by_head):
        per_head = pl.BlockSpec((1, tok_rows, head_size), lambda k: (k + first, 0, 0))
        acc_spec = pl.BlockSpec((1, blocks_here, head_size, rows), lambda k: (k + first, 0, 0, 0))
        row_spec = pl.BlockSpec((1, blocks_here, 1, rows), lambda k: (k + first, 0, 0, 0))
        whole = [pl.BlockSpec(memory_space=pl.ANY)] * len(state)
        return pl.pallas_call(
            lambda *refs: window_kernel(*refs, scale=scale),
            grid=(count,),
            in_specs=[
                pl.BlockSpec(memory_space=pltpu.SMEM),
                pl.BlockSpec((blocks_here, 1, rows), lambda k: (0, 0, 0)),
                pl.BlockSpec((group, tok_rows, head_size), lambda k: (k + first, 0, 0)),
                *[per_head] * 4, *whole,
            ],
            out_specs=[acc_spec, row_spec, row_spec],
            out_shape=[acc_shape, row_shape, row_shape],
            input_output_aliases={7 + i: i for i in range(len(state))},
            cost_estimate=pl.CostEstimate(
                flops=4 * work * count * head_size,
                bytes_accessed=count << 20,
                transcendentals=work * count,
            ),
            compiler_params=pltpu.CompilerParams(vmem_limit_bytes=16 << 20),
            name=f"window_heads_{first}",
        )(rank.reshape(1), ready["low"], by_head, *ready["near"], mine, rest, *state)

    def beside(first, count):
        def run(before, results):
            nonlocal state
            by_head, _ = lax.optimization_barrier((ready["by_head"], before))
            state = window_part(first, count, by_head)
            *results, acc, peak, total = lax.optimization_barrier((*results, *state))
            state = [acc, peak, total]
            return results

        return run

    quarter = kv_count // 4
    besides = [send_near, lay_queries, beside(0, quarter), beside(quarter, 2 * quarter)]
    besides.append(beside(3 * quarter, quarter))
    own, other = gather_globals(mine, twin, global_ids, besides)
    place = [0] * side
    for at, offset in enumerate(HELD):
        place[offset % side] = at
    pair = 2
    whole = pl.BlockSpec((kv_count, slots * BLK, head_size), lambda k, *_: (0, 0, 0))
    acc_spec = pl.BlockSpec((pair, blocks_here, head_size, rows), lambda k, *_: (k, 0, 0, 0))
    row_spec = pl.BlockSpec((pair, blocks_here, 1, rows), lambda k, *_: (k, 0, 0, 0))
    return pl.pallas_call(
        lambda *refs: global_kernel(*refs, scale=scale),
        grid_spec=pltpu.PrefetchScalarGridSpec(
            num_scalar_prefetch=3,
            grid=(kv_count // pair,),
            in_specs=[
                pl.BlockSpec((pair * group, tok_rows, head_size), lambda k, *_: (k, 0, 0)),
                whole, whole, acc_spec, row_spec, row_spec,
            ],
            out_specs=pl.BlockSpec((tok_rows, pair * group, head_size), lambda k, *_: (0, k, 0)),
        ),
        out_shape=jax.ShapeDtypeStruct((tok_rows, heads_here, head_size), jnp.bfloat16),
        compiler_params=pltpu.CompilerParams(vmem_limit_bytes=32 << 20),
        name="global_part",
    )(jnp.array(place, jnp.int32), rank.reshape(1), global_ids, ready["by_head"], own, other, *state)


def solution(mesh):
    shard = P(("grp", "seq"), None, None)
    return jax.shard_map(
        per_device,
        mesh=mesh,
        in_specs=(shard, shard, shard, P("grp"), P("grp")),
        out_specs=shard,
        check_vma=False,
    )
```

```python
import math

import jax
import jax.numpy as jnp
from jax import lax
from jax.experimental import pallas as pl
from jax.experimental.pallas import tpu as pltpu
from jax.sharding import PartitionSpec as P

BLK = 128
WIN = 3
masked_score = -1e30

HELD = (0, -3, 3, -1, -4, 2, 1, -2)

SEATS = 2


def ring_pairs(side, core0, core1):
    pairs = []
    for x in range(side):
        for y in range(side):
            for core, (dx, dy) in enumerate((core0, core1)):
                to = ((x + dx) % side) * side + (y + dy) % side
                pairs.append(((x * side + y) * 2 + core, to * 2 + core))
    return pairs


def along_scatter(shard, side, by):
    return lax.ppermute(shard, "seq", ring_pairs(side, (0, by), (by, 0)))


def across_scatter(shard, side, by):
    return lax.ppermute(shard, "seq", ring_pairs(side, (by, 0), (0, by)))


def pick(flag, one, other):
    return jnp.where(flag[:, None, None], one, other)


def owner_of(ids, slot, blocks_chip):
    return lax.div(ids[slot], blocks_chip)


def turn_of(ids, slot, blocks_chip):
    owner = owner_of(ids, slot, blocks_chip)
    return sum((owner_of(ids, s, blocks_chip) == owner).astype(jnp.int32) for s in range(slot))


def pick_kernel(rank_ref, ids, turn_ref, mine_ref, twin_ref, out_ref, rounds_ref):
    blocks_here = mine_ref.shape[1] // BLK
    blocks_chip = 2 * blocks_here
    chip, core = lax.div(rank_ref[0], 2), lax.rem(rank_ref[0], 2)
    last = jnp.int32(0)
    for slot in range(1, ids.shape[0]):
        last = jnp.maximum(last, turn_of(ids, slot, blocks_chip))
    rounds_ref[0] = lax.div(last, SEATS)
    for lane in range(SEATS):
        count, local = jnp.int32(0), jnp.int32(0)
        for slot in range(ids.shape[0]):
            on_chip = owner_of(ids, slot, blocks_chip) == chip
            hit = on_chip & (count == turn_ref[0] * SEATS + lane)
            local = jnp.where(hit, lax.rem(ids[slot], blocks_chip), local)
            count = count + on_chip.astype(jnp.int32)
        from_mine = lax.div(local, blocks_here) == core
        start = pl.multiple_of(lax.rem(local, blocks_here) * BLK, BLK)
        to = pl.ds(lane * BLK, BLK)

        @pl.when(from_mine)
        def _():
            out_ref[:, to, :] = mine_ref[:, pl.ds(start, BLK), :]

        @pl.when(jnp.logical_not(from_mine))
        def _():
            out_ref[:, to, :] = twin_ref[:, pl.ds(start, BLK), :]


def seat_kernel(rank_ref, ids, turn_ref, parts_ref, *refs, blocks_chip, side):
    is0 = lax.rem(rank_ref[0], 2) == 0
    for slot in range(ids.shape[0]):
        owner = owner_of(ids, slot, blocks_chip)
        source = jnp.where(is0, lax.rem(owner, side), lax.div(owner, side))
        turn = turn_of(ids, slot, blocks_chip)
        start = pl.multiple_of(lax.rem(turn, SEATS) * BLK, BLK)
        part = parts_ref[source, pl.ds(start, BLK), :]
        if len(refs) > 1:
            part = jnp.where(lax.div(turn, SEATS) == turn_ref[0], part, refs[0][slot])
        refs[-1][slot] = part


def gather_globals(mine, twin, global_ids, besides):
    devices = lax.axis_size("seq")
    side = math.isqrt(devices // 2)
    rank = lax.axis_index("seq")
    core, chip = rank % 2, rank // 2
    x, y = chip // side, chip % side
    heads, tok_rows, head_size = mine.shape
    slots = global_ids.shape[0]
    blocks_chip = 2 * (tok_rows // BLK)
    owner = global_ids // blocks_chip
    is0 = core == 0
    cross_pos = jnp.where(is0, x, y)
    owner_cross = jnp.where(is0, owner // side, owner % side)
    groups = [[(i * side + j) * 2 for j in range(side)] for i in range(side)]
    groups += [[(j * side + i) * 2 + 1 for j in range(side)] for i in range(side)]
    swap = [(i, i ^ 1) for i in range(devices)]
    scalars = [pl.BlockSpec(memory_space=pltpu.SMEM)] * 3
    vmem = pl.BlockSpec(memory_space=pltpu.VMEM)
    small = pltpu.CompilerParams(vmem_limit_bytes=16 << 20)

    def scatter(turn, held, run):
        spot = (rank.reshape(1), global_ids, turn.reshape(1))
        part, rounds = pl.pallas_call(
            pick_kernel,
            in_specs=[*scalars, vmem, vmem],
            out_specs=[vmem, scalars[0]],
            out_shape=[
                jax.ShapeDtypeStruct((heads, SEATS * BLK, head_size), mine.dtype),
                jax.ShapeDtypeStruct((1,), jnp.int32),
            ],
            compiler_params=small,
            name="pick",
        )(*spot, mine, twin)
        parts = lax.all_to_all(part, "seq", 0, 0, axis_index_groups=groups, tiled=True)
        parts = run(part, parts)
        held = pl.pallas_call(
            lambda *refs: seat_kernel(*refs, blocks_chip=blocks_chip, side=side),
            in_specs=[*scalars, vmem, *[vmem] * len(held)],
            out_specs=vmem,
            out_shape=jax.ShapeDtypeStruct((slots, BLK, head_size), mine.dtype),
            compiler_params=small,
            name="seat",
        )(*spot, parts, *held)
        return held, rounds[0]

    held, last_turn = scatter(jnp.int32(0), [], besides[0])
    _, held = lax.while_loop(
        lambda carried: carried[0] > 0,
        lambda carried: (carried[0] - 1, scatter(carried[0], carried[1:], lambda _, parts: parts)[0]),
        (last_turn, held),
    )
    away = (owner_cross - cross_pos) % side
    before = held
    down, up = across_scatter(held, side, 3), across_scatter(held, side, -3)
    down, up = besides[1](before, (down, up))
    held = pick(away == side - 3, down, pick(away == 3, up, held))
    before = held
    down, up = across_scatter(held, side, 1), across_scatter(held, side, -1)
    down, up = besides[2](before, (down, up))
    from_down = (away == side - 1) | (away == side // 2) | (away == 2)
    from_up = (away == 1) | (away == side - 2)
    held = pick(from_down, down, pick(from_up, up, held))
    before = held
    down, up = along_scatter(held, side, 3), along_scatter(held, side, -3)
    down, up = besides[3](before, (down, up))
    three = jnp.stack([held, down, up])
    before = three
    down, up = along_scatter(three, side, 1), along_scatter(three[:2], side, -1)
    down, up = besides[4](before, (down, up))
    own = jnp.concatenate([three, down, up]).reshape(heads, slots * BLK, head_size)
    other = lax.ppermute(own, "seq", swap)
    return own, other


def over_keys(one, two):
    return lax.dot_general(one, two, (((0,), (0,)), ((), ())), preferred_element_type=jnp.float32)


def over_head(one, two):
    return lax.dot_general(one, two, (((1,), (1,)), ((), ())), preferred_element_type=jnp.float32)


def window_kernel(rank_ref, low_ref, q_ref, near, mine, rest, *refs, scale):
    acc_ref, peak_ref, sum_ref = refs[-3:]
    group, tok_rows, head_size = q_ref.shape
    is0 = lax.rem(rank_ref[0], 2) == 0
    near_a, near_b, own_a, own_b = near[0, 0], near[1, 0], mine[0], rest[0]
    keys = [jnp.where(is0, near_b, near_a), jnp.where(is0, own_a, own_b)]
    vals = [jnp.where(is0, near_a, near_b), jnp.where(is0, own_b, own_a)]
    keys, vals = jnp.concatenate(keys, axis=0), jnp.concatenate(vals, axis=0)
    span = WIN * BLK
    rows = group * BLK
    for b in range(tok_rows // BLK):
        queries = q_ref[:, b * BLK : (b + 1) * BLK, :].reshape(rows, head_size)
        scores = over_head(keys[b * BLK : b * BLK + span], queries) * scale
        key_at = lax.broadcasted_iota(jnp.int32, (span, rows), 0) + b * BLK
        query_at = lax.broadcasted_iota(jnp.int32, (1, rows), 1) % BLK + (tok_rows + b * BLK)
        allowed = (key_at >= low_ref[b]) & (key_at <= query_at)
        scores = jnp.where(allowed, scores, masked_score)
        peak = jnp.max(scores, axis=0, keepdims=True)
        terms = jnp.exp2(scores - peak)
        sum_ref[0, b] = jnp.sum(terms, axis=0, keepdims=True)
        peak_ref[0, b] = peak
        acc_ref[0, b] = over_keys(vals[b * BLK : b * BLK + span], terms.astype(jnp.bfloat16))


def global_kernel(
    place, rank_ref, ids, q_ref, own_ref, other_ref, acc_ref, peak_ref, sum_ref, out_ref, *, scale
):
    kv_count, blocks_here, head_size, rows = acc_ref.shape
    pair = out_ref.shape[1] * BLK // rows
    side = place.shape[0]
    group = rows // BLK
    slots = ids.shape[0]
    rank = rank_ref[0]
    chip = lax.div(rank, 2)
    x, y = lax.div(chip, side), lax.rem(chip, side)
    is0 = lax.rem(rank, 2) == 0
    first = pl.program_id(0) * pair
    gap_bias = []
    for b in range(blocks_here):
        gaps = [rank * blocks_here + b - ids[s] for s in range(slots)]
        gap_bias.append([jnp.where((g >= 0) & (g < WIN), masked_score, 0.0) for g in gaps])
    pairs = []
    for j in range(pair):
        key_at = place[lax.rem(first + j - y + side, side)]
        val_at = place[lax.rem(first + j - x + side, side)]
        pairs.append((
            jnp.where(is0, own_ref[key_at], other_ref[key_at]),
            jnp.where(is0, other_ref[val_at], own_ref[val_at]),
        ))
    for b in range(blocks_here):
        outs = []
        for j, (keys, vals) in enumerate(pairs):
            head = pl.ds((first + j) * group, group)
            queries = q_ref[head, b * BLK : (b + 1) * BLK, :]
            scores = over_head(keys, queries.reshape(rows, head_size)) * scale
            before = peak_ref[first + j, b]
            peak = before
            parts = [scores[s * BLK : (s + 1) * BLK] for s in range(slots)]
            for s in range(slots):
                top = jnp.max(parts[s], axis=0, keepdims=True)
                peak = jnp.maximum(peak, top + gap_bias[b][s])
            factor = jnp.exp2(before - peak)
            total = sum_ref[first + j, b] * factor
            terms = []
            for s in range(slots):
                term = jnp.exp2(parts[s] - (peak - gap_bias[b][s]))
                total = total + jnp.sum(term, axis=0, keepdims=True)
                terms.append(term.astype(jnp.bfloat16))
            acc = acc_ref[first + j, b] * factor + over_keys(vals, jnp.concatenate(terms, axis=0))
            outs.append((acc * (1.0 / total)).T.reshape(group, BLK, head_size))
        rows_out = jnp.transpose(jnp.concatenate(outs, axis=0), (1, 0, 2))
        out_ref[b * BLK : (b + 1) * BLK] = rows_out.astype(out_ref.dtype)


def per_device(queries, keys, values, global_ids, doc_lengths):
    tok_rows, heads_here, head_size = queries.shape
    kv_count = keys.shape[1]
    group = heads_here // kv_count
    blocks_here = tok_rows // BLK
    rows = group * BLK
    slots = global_ids.shape[0]
    scale = math.log2(math.e) / math.sqrt(head_size)
    rank = lax.axis_index("seq")
    devices = lax.axis_size("seq")
    side = math.isqrt(devices // 2)
    first_pos = rank * tok_rows
    doc_ends = jnp.cumsum(doc_lengths)
    query_pos = first_pos + jnp.arange(tok_rows, dtype=jnp.int32)
    is0 = rank % 2 == 0
    mine = jnp.where(is0, keys, values).transpose(1, 0, 2)
    rest = jnp.where(is0, values, keys).transpose(1, 0, 2)
    twin = lax.ppermute(rest, "seq", [(i, i ^ 1) for i in range(devices)])

    acc_shape = jax.ShapeDtypeStruct((kv_count, blocks_here, head_size, rows), jnp.float32)
    row_shape = jax.ShapeDtypeStruct((kv_count, blocks_here, 1, rows), jnp.float32)
    work = blocks_here * rows * BLK * WIN
    ring = [(i, i + 1) for i in range(devices - 1)]
    ready, state = {}, []

    def send_near(before, result):
        mine_now, rest_now, ends, _ = lax.optimization_barrier((mine, rest, doc_ends, before))
        begun = ends[None, :] <= query_pos[:, None]
        low = jnp.max(jnp.where(begun, ends[None, :], 0), axis=1) - (first_pos - tok_rows)
        low = jnp.tile(low.reshape(blocks_here, 1, BLK), (1, 1, group))
        near = lax.ppermute(jnp.stack([mine_now, rest_now]), "seq", ring)
        result, low = lax.optimization_barrier((result, low))
        ready.update(low=low, near=near)
        return result

    def lay_queries(before, results):
        given, _ = lax.optimization_barrier((queries, before))
        *results, by_head = lax.optimization_barrier((*results, given.transpose(1, 0, 2)))
        ready.update(by_head=by_head)
        return results

    def window_part(first, count, by_head):
        per_head = pl.BlockSpec((1, tok_rows, head_size), lambda k: (k + first, 0, 0))
        acc_spec = pl.BlockSpec((1, blocks_here, head_size, rows), lambda k: (k + first, 0, 0, 0))
        row_spec = pl.BlockSpec((1, blocks_here, 1, rows), lambda k: (k + first, 0, 0, 0))
        whole = [pl.BlockSpec(memory_space=pl.ANY)] * len(state)
        return pl.pallas_call(
            lambda *refs: window_kernel(*refs, scale=scale),
            grid=(count,),
            in_specs=[
                pl.BlockSpec(memory_space=pltpu.SMEM),
                pl.BlockSpec((blocks_here, 1, rows), lambda k: (0, 0, 0)),
                pl.BlockSpec((group, tok_rows, head_size), lambda k: (k + first, 0, 0)),
                pl.BlockSpec((2, 1, tok_rows, head_size), lambda k: (0, k + first, 0, 0)),
                per_head, per_head, *whole,
            ],
            out_specs=[acc_spec, row_spec, row_spec],
            out_shape=[acc_shape, row_shape, row_shape],
            input_output_aliases={6 + i: i for i in range(len(state))},
            cost_estimate=pl.CostEstimate(
                flops=4 * work * count * head_size,
                bytes_accessed=count << 20,
                transcendentals=work * count,
            ),
            compiler_params=pltpu.CompilerParams(vmem_limit_bytes=16 << 20),
            name=f"window_heads_{first}",
        )(rank.reshape(1), ready["low"], by_head, ready["near"], mine, rest, *state)

    def beside(first, count):
        def run(before, results):
            nonlocal state
            by_head, _ = lax.optimization_barrier((ready["by_head"], before))
            state = window_part(first, count, by_head)
            *results, acc, peak, total = lax.optimization_barrier((*results, *state))
            state = [acc, peak, total]
            return results

        return run

    quarter = kv_count // 4
    besides = [send_near, lay_queries, beside(0, quarter), beside(quarter, 2 * quarter)]
    besides.append(beside(3 * quarter, quarter))
    own, other = gather_globals(mine, twin, global_ids, besides)
    place = [0] * side
    for at, offset in enumerate(HELD):
        place[offset % side] = at
    pair = 2
    whole = pl.BlockSpec(memory_space=pltpu.VMEM)
    return pl.pallas_call(
        lambda *refs: global_kernel(*refs, scale=scale),
        grid_spec=pltpu.PrefetchScalarGridSpec(
            num_scalar_prefetch=3,
            grid=(kv_count // pair,),
            in_specs=[whole] * 6,
            out_specs=pl.BlockSpec((tok_rows, pair * group, head_size), lambda k, *_: (0, k, 0)),
        ),
        out_shape=jax.ShapeDtypeStruct((tok_rows, heads_here, head_size), jnp.bfloat16),
        compiler_params=pltpu.CompilerParams(vmem_limit_bytes=32 << 20),
        name="global_part",
    )(jnp.array(place, jnp.int32), rank.reshape(1), global_ids, ready["by_head"], own, other, *state)


def solution(mesh):
    shard = P(("grp", "seq"), None, None)
    return jax.shard_map(
        per_device,
        mesh=mesh,
        in_specs=(shard, shard, shard, P("grp"), P("grp")),
        out_specs=shard,
        check_vma=False,
    )
```

```python
import math

import jax
import jax.numpy as jnp
from jax import lax
from jax.experimental import pallas as pl
from jax.experimental.pallas import tpu as pltpu
from jax.sharding import PartitionSpec as P

BLK = 128
WIN = 3
masked_score = -1e30

HELD = (0, -3, 3, -1, -4, 2, 1, -2)

SEATS = 2


def ring_pairs(side, core0, core1):
    pairs = []
    for x in range(side):
        for y in range(side):
            for core, (dx, dy) in enumerate((core0, core1)):
                to = ((x + dx) % side) * side + (y + dy) % side
                pairs.append(((x * side + y) * 2 + core, to * 2 + core))
    return pairs


def along_scatter(shard, side, by):
    return lax.ppermute(shard, "seq", ring_pairs(side, (0, by), (by, 0)))


def across_scatter(shard, side, by):
    return lax.ppermute(shard, "seq", ring_pairs(side, (by, 0), (0, by)))


def pick(flag, one, other):
    return jnp.where(flag[:, None, None], one, other)


def owner_of(ids, slot, blocks_chip):
    return lax.div(ids[slot], blocks_chip)


def turn_of(ids, slot, blocks_chip):
    owner = owner_of(ids, slot, blocks_chip)
    return sum((owner_of(ids, s, blocks_chip) == owner).astype(jnp.int32) for s in range(slot))


def pick_kernel(rank_ref, ids, turn_ref, mine_ref, twin_ref, out_ref, rounds_ref):
    blocks_here = mine_ref.shape[1] // BLK
    blocks_chip = 2 * blocks_here
    chip, core = lax.div(rank_ref[0], 2), lax.rem(rank_ref[0], 2)
    last = jnp.int32(0)
    for slot in range(1, ids.shape[0]):
        last = jnp.maximum(last, turn_of(ids, slot, blocks_chip))
    rounds_ref[0] = lax.div(last, SEATS)
    for lane in range(SEATS):
        count, local = jnp.int32(0), jnp.int32(0)
        for slot in range(ids.shape[0]):
            on_chip = owner_of(ids, slot, blocks_chip) == chip
            hit = on_chip & (count == turn_ref[0] * SEATS + lane)
            local = jnp.where(hit, lax.rem(ids[slot], blocks_chip), local)
            count = count + on_chip.astype(jnp.int32)
        from_mine = lax.div(local, blocks_here) == core
        start = pl.multiple_of(lax.rem(local, blocks_here) * BLK, BLK)
        to = pl.ds(lane * BLK, BLK)

        @pl.when(from_mine)
        def _():
            out_ref[:, to, :] = mine_ref[:, pl.ds(start, BLK), :]

        @pl.when(jnp.logical_not(from_mine))
        def _():
            out_ref[:, to, :] = twin_ref[:, pl.ds(start, BLK), :]


def seat_kernel(rank_ref, ids, turn_ref, parts_ref, *refs, blocks_chip, side):
    is0 = lax.rem(rank_ref[0], 2) == 0
    for slot in range(ids.shape[0]):
        owner = owner_of(ids, slot, blocks_chip)
        source = jnp.where(is0, lax.rem(owner, side), lax.div(owner, side))
        turn = turn_of(ids, slot, blocks_chip)
        start = pl.multiple_of(lax.rem(turn, SEATS) * BLK, BLK)
        part = parts_ref[source, pl.ds(start, BLK), :]
        if len(refs) > 1:
            part = jnp.where(lax.div(turn, SEATS) == turn_ref[0], part, refs[0][slot])
        refs[-1][slot] = part


def gather_globals(mine, twin, global_ids, besides):
    devices = lax.axis_size("seq")
    side = math.isqrt(devices // 2)
    rank = lax.axis_index("seq")
    core, chip = rank % 2, rank // 2
    x, y = chip // side, chip % side
    heads, tok_rows, head_size = mine.shape
    slots = global_ids.shape[0]
    blocks_chip = 2 * (tok_rows // BLK)
    owner = global_ids // blocks_chip
    is0 = core == 0
    cross_pos = jnp.where(is0, x, y)
    owner_cross = jnp.where(is0, owner // side, owner % side)
    groups = [[(i * side + j) * 2 for j in range(side)] for i in range(side)]
    groups += [[(j * side + i) * 2 + 1 for j in range(side)] for i in range(side)]
    swap = [(i, i ^ 1) for i in range(devices)]
    scalars = [pl.BlockSpec(memory_space=pltpu.SMEM)] * 3
    vmem = pl.BlockSpec(memory_space=pltpu.VMEM)
    small = pltpu.CompilerParams(vmem_limit_bytes=16 << 20)

    def scatter(turn, held, run):
        spot = (rank.reshape(1), global_ids, turn.reshape(1))
        part, rounds = pl.pallas_call(
            pick_kernel,
            in_specs=[*scalars, vmem, vmem],
            out_specs=[vmem, scalars[0]],
            out_shape=[
                jax.ShapeDtypeStruct((heads, SEATS * BLK, head_size), mine.dtype),
                jax.ShapeDtypeStruct((1,), jnp.int32),
            ],
            compiler_params=small,
            name="pick",
        )(*spot, mine, twin)
        parts = lax.all_to_all(part, "seq", 0, 0, axis_index_groups=groups, tiled=True)
        parts = run(part, parts)
        held = pl.pallas_call(
            lambda *refs: seat_kernel(*refs, blocks_chip=blocks_chip, side=side),
            in_specs=[*scalars, vmem, *[vmem] * len(held)],
            out_specs=vmem,
            out_shape=jax.ShapeDtypeStruct((slots, BLK, head_size), mine.dtype),
            compiler_params=small,
            name="seat",
        )(*spot, parts, *held)
        return held, rounds[0]

    held, last_turn = scatter(jnp.int32(0), [], besides[0])
    _, held = lax.while_loop(
        lambda carried: carried[0] > 0,
        lambda carried: (carried[0] - 1, scatter(carried[0], carried[1:], lambda _, parts: parts)[0]),
        (last_turn, held),
    )
    away = (owner_cross - cross_pos) % side
    before = held
    down, up = across_scatter(held, side, 3), across_scatter(held, side, -3)
    down, up = besides[1](before, (down, up))
    held = pick(away == side - 3, down, pick(away == 3, up, held))
    before = held
    down, up = across_scatter(held, side, 1), across_scatter(held, side, -1)
    down, up = besides[2](before, (down, up))
    from_down = (away == side - 1) | (away == side // 2) | (away == 2)
    from_up = (away == 1) | (away == side - 2)
    held = pick(from_down, down, pick(from_up, up, held))
    before = held
    down, up = along_scatter(held, side, 3), along_scatter(held, side, -3)
    down, up = besides[3](before, (down, up))
    three = jnp.stack([held, down, up])
    before = three
    down, up = along_scatter(three, side, 1), along_scatter(three[:2], side, -1)
    down, up = besides[4](before, (down, up))
    own = jnp.concatenate([three, down, up]).reshape(heads, slots * BLK, head_size)
    other = lax.ppermute(own, "seq", swap)
    return own, other


def over_keys(one, two):
    return lax.dot_general(one, two, (((0,), (0,)), ((), ())), preferred_element_type=jnp.float32)


def over_head(one, two):
    return lax.dot_general(one, two, (((1,), (1,)), ((), ())), preferred_element_type=jnp.float32)


def window_kernel(rank_ref, low_ref, q_ref, near, mine, rest, *refs, scale):
    acc_ref, peak_ref, sum_ref = refs[-3:]
    group, tok_rows, head_size = q_ref.shape
    is0 = lax.rem(rank_ref[0], 2) == 0
    near_a, near_b, own_a, own_b = near[0, 0], near[1, 0], mine[0], rest[0]
    keys = [jnp.where(is0, near_b, near_a), jnp.where(is0, own_a, own_b)]
    vals = [jnp.where(is0, near_a, near_b), jnp.where(is0, own_b, own_a)]
    keys, vals = jnp.concatenate(keys, axis=0), jnp.concatenate(vals, axis=0)
    span = WIN * BLK
    rows = group * BLK
    for b in range(tok_rows // BLK):
        queries = q_ref[:, b * BLK : (b + 1) * BLK, :].reshape(rows, head_size)
        scores = over_head(keys[b * BLK : b * BLK + span], queries) * scale
        key_at = lax.broadcasted_iota(jnp.int32, (span, rows), 0) + b * BLK
        query_at = lax.broadcasted_iota(jnp.int32, (1, rows), 1) % BLK + (tok_rows + b * BLK)
        allowed = (key_at >= low_ref[b]) & (key_at <= query_at)
        scores = jnp.where(allowed, scores, masked_score)
        peak = jnp.max(scores, axis=0, keepdims=True)
        terms = jnp.exp2(scores - peak)
        sum_ref[0, b] = jnp.sum(terms, axis=0, keepdims=True)
        peak_ref[0, b] = peak
        acc_ref[0, b] = over_keys(vals[b * BLK : b * BLK + span], terms.astype(jnp.bfloat16))


def global_kernel(
    place, rank_ref, ids, q_ref, own_ref, other_ref, acc_ref, peak_ref, sum_ref, out_ref,
    *score_refs, scale,
):
    kv_count, blocks_here, head_size, rows = acc_ref.shape
    pair = score_refs[0].shape[0]
    side = place.shape[0]
    group = rows // BLK
    slots = ids.shape[0]
    rank = rank_ref[0]
    chip = lax.div(rank, 2)
    x, y = lax.div(chip, side), lax.rem(chip, side)
    is0 = lax.rem(rank, 2) == 0
    step = pl.program_id(0)

    def score(step, b):
        for j in range(pair):
            head = step * pair + j
            at = place[lax.rem(head - y + side, side)]
            keys = jnp.where(is0, own_ref[at], other_ref[at])
            queries = q_ref[pl.ds(head * group, group), b * BLK : (b + 1) * BLK, :]
            score_refs[b][j] = over_head(keys, queries.reshape(rows, head_size))

    def attend(step, b):
        gaps = [rank * blocks_here + b - ids[s] for s in range(slots)]
        bias = [jnp.where((g >= 0) & (g < WIN), masked_score, 0.0) for g in gaps]
        outs = []
        for j in range(pair):
            head = step * pair + j
            at = place[lax.rem(head - x + side, side)]
            vals = jnp.where(is0, other_ref[at], own_ref[at])
            before = peak_ref[head, b]
            peak = before
            for s in range(slots):
                top = jnp.max(score_refs[b][j, s * BLK : (s + 1) * BLK], axis=0, keepdims=True)
                peak = jnp.maximum(peak, top * scale + bias[s])
            factor = jnp.exp2(before - peak)
            total = sum_ref[head, b] * factor
            terms = []
            for s in range(slots):
                part = score_refs[b][j, s * BLK : (s + 1) * BLK]
                term = jnp.exp2(part * scale - (peak - bias[s]))
                total = total + jnp.sum(term, axis=0, keepdims=True)
                terms.append(term.astype(jnp.bfloat16))
            acc = acc_ref[head, b] * factor + over_keys(vals, jnp.concatenate(terms, axis=0))
            outs.append((acc * (1.0 / total)).T.reshape(group, BLK, head_size))
        rows_out = jnp.transpose(jnp.concatenate(outs, axis=0), (1, 0, 2))
        out_ref[b * BLK : (b + 1) * BLK] = rows_out.astype(out_ref.dtype)

    @pl.when(step == 0)
    def _():
        score(step, 0)

    for b in range(blocks_here):
        attend(step, b)
        if b + 1 < blocks_here:
            score(step, b + 1)
        else:
            score(jnp.minimum(step + 1, pl.num_programs(0) - 1), 0)


def per_device(queries, keys, values, global_ids, doc_lengths):
    tok_rows, heads_here, head_size = queries.shape
    kv_count = keys.shape[1]
    group = heads_here // kv_count
    blocks_here = tok_rows // BLK
    rows = group * BLK
    slots = global_ids.shape[0]
    scale = math.log2(math.e) / math.sqrt(head_size)
    rank = lax.axis_index("seq")
    devices = lax.axis_size("seq")
    side = math.isqrt(devices // 2)
    first_pos = rank * tok_rows
    doc_ends = jnp.cumsum(doc_lengths)
    query_pos = first_pos + jnp.arange(tok_rows, dtype=jnp.int32)
    is0 = rank % 2 == 0
    mine = jnp.where(is0, keys, values).transpose(1, 0, 2)
    rest = jnp.where(is0, values, keys).transpose(1, 0, 2)
    twin = lax.ppermute(rest, "seq", [(i, i ^ 1) for i in range(devices)])

    acc_shape = jax.ShapeDtypeStruct((kv_count, blocks_here, head_size, rows), jnp.float32)
    row_shape = jax.ShapeDtypeStruct((kv_count, blocks_here, 1, rows), jnp.float32)
    work = blocks_here * rows * BLK * WIN
    ring = [(i, i + 1) for i in range(devices - 1)]
    ready, state = {}, []

    def send_near(before, result):
        mine_now, rest_now, ends, _ = lax.optimization_barrier((mine, rest, doc_ends, before))
        begun = ends[None, :] <= query_pos[:, None]
        low = jnp.max(jnp.where(begun, ends[None, :], 0), axis=1) - (first_pos - tok_rows)
        low = jnp.tile(low.reshape(blocks_here, 1, BLK), (1, 1, group))
        near = lax.ppermute(jnp.stack([mine_now, rest_now]), "seq", ring)
        result, low = lax.optimization_barrier((result, low))
        ready.update(low=low, near=near)
        return result

    def lay_queries(before, results):
        given, _ = lax.optimization_barrier((queries, before))
        *results, by_head = lax.optimization_barrier((*results, given.transpose(1, 0, 2)))
        ready.update(by_head=by_head)
        return results

    def window_part(first, count, by_head):
        per_head = pl.BlockSpec((1, tok_rows, head_size), lambda k: (k + first, 0, 0))
        acc_spec = pl.BlockSpec((1, blocks_here, head_size, rows), lambda k: (k + first, 0, 0, 0))
        row_spec = pl.BlockSpec((1, blocks_here, 1, rows), lambda k: (k + first, 0, 0, 0))
        whole = [pl.BlockSpec(memory_space=pl.ANY)] * len(state)
        return pl.pallas_call(
            lambda *refs: window_kernel(*refs, scale=scale),
            grid=(count,),
            in_specs=[
                pl.BlockSpec(memory_space=pltpu.SMEM),
                pl.BlockSpec((blocks_here, 1, rows), lambda k: (0, 0, 0)),
                pl.BlockSpec((group, tok_rows, head_size), lambda k: (k + first, 0, 0)),
                pl.BlockSpec((2, 1, tok_rows, head_size), lambda k: (0, k + first, 0, 0)),
                per_head, per_head, *whole,
            ],
            out_specs=[acc_spec, row_spec, row_spec],
            out_shape=[acc_shape, row_shape, row_shape],
            input_output_aliases={6 + i: i for i in range(len(state))},
            cost_estimate=pl.CostEstimate(
                flops=4 * work * count * head_size,
                bytes_accessed=count << 20,
                transcendentals=work * count,
            ),
            compiler_params=pltpu.CompilerParams(vmem_limit_bytes=16 << 20),
            name=f"window_heads_{first}",
        )(rank.reshape(1), ready["low"], by_head, ready["near"], mine, rest, *state)

    def beside(first, count):
        def run(before, results):
            nonlocal state
            by_head, _ = lax.optimization_barrier((ready["by_head"], before))
            state = window_part(first, count, by_head)
            *results, acc, peak, total = lax.optimization_barrier((*results, *state))
            state = [acc, peak, total]
            return results

        return run

    quarter = kv_count // 4
    besides = [send_near, lay_queries, beside(0, quarter), beside(quarter, 2 * quarter)]
    besides.append(beside(3 * quarter, quarter))
    own, other = gather_globals(mine, twin, global_ids, besides)
    place = [0] * side
    for at, offset in enumerate(HELD):
        place[offset % side] = at
    pair = 2
    whole = pl.BlockSpec(memory_space=pltpu.VMEM)
    return pl.pallas_call(
        lambda *refs: global_kernel(*refs, scale=scale),
        grid_spec=pltpu.PrefetchScalarGridSpec(
            num_scalar_prefetch=3,
            grid=(kv_count // pair,),
            in_specs=[whole] * 6,
            out_specs=pl.BlockSpec((tok_rows, pair * group, head_size), lambda k, *_: (0, k, 0)),
            scratch_shapes=[pltpu.VMEM((pair, slots * BLK, rows), jnp.float32)] * blocks_here,
        ),
        out_shape=jax.ShapeDtypeStruct((tok_rows, heads_here, head_size), jnp.bfloat16),
        compiler_params=pltpu.CompilerParams(vmem_limit_bytes=32 << 20),
        name="global_part",
    )(jnp.array(place, jnp.int32), rank.reshape(1), global_ids, ready["by_head"], own, other, *state)


def solution(mesh):
    shard = P(("grp", "seq"), None, None)
    return jax.shard_map(
        per_device,
        mesh=mesh,
        in_specs=(shard, shard, shard, P("grp"), P("grp")),
        out_specs=shard,
        check_vma=False,
    )
```

```python
import math

import jax
import jax.numpy as jnp
from jax import lax
from jax.experimental import pallas as pl
from jax.experimental.pallas import tpu as pltpu
from jax.sharding import PartitionSpec as P

BLK = 128
WIN = 3
masked_score = -1e30

HELD = (0, -3, 3, -1, -4, 2, 1, -2)

SEATS = 2


def ring_pairs(side, core0, core1):
    pairs = []
    for x in range(side):
        for y in range(side):
            for core, (dx, dy) in enumerate((core0, core1)):
                to = ((x + dx) % side) * side + (y + dy) % side
                pairs.append(((x * side + y) * 2 + core, to * 2 + core))
    return pairs


def along_scatter(shard, side, by):
    return lax.ppermute(shard, "seq", ring_pairs(side, (0, by), (by, 0)))


def across_scatter(shard, side, by):
    return lax.ppermute(shard, "seq", ring_pairs(side, (by, 0), (0, by)))


def pick(flag, one, other):
    return jnp.where(flag[:, None, None], one, other)


def owner_of(ids, slot, blocks_chip):
    return lax.div(ids[slot], blocks_chip)


def turn_of(ids, slot, blocks_chip):
    owner = owner_of(ids, slot, blocks_chip)
    return sum((owner_of(ids, s, blocks_chip) == owner).astype(jnp.int32) for s in range(slot))


def pick_kernel(rank_ref, ids, turn_ref, mine_ref, twin_ref, out_ref, rounds_ref):
    blocks_here = mine_ref.shape[1] // BLK
    blocks_chip = 2 * blocks_here
    chip, core = lax.div(rank_ref[0], 2), lax.rem(rank_ref[0], 2)
    last = jnp.int32(0)
    for slot in range(1, ids.shape[0]):
        last = jnp.maximum(last, turn_of(ids, slot, blocks_chip))
    rounds_ref[0] = lax.div(last, SEATS)
    for lane in range(SEATS):
        count, local = jnp.int32(0), jnp.int32(0)
        for slot in range(ids.shape[0]):
            on_chip = owner_of(ids, slot, blocks_chip) == chip
            hit = on_chip & (count == turn_ref[0] * SEATS + lane)
            local = jnp.where(hit, lax.rem(ids[slot], blocks_chip), local)
            count = count + on_chip.astype(jnp.int32)
        from_mine = lax.div(local, blocks_here) == core
        start = pl.multiple_of(lax.rem(local, blocks_here) * BLK, BLK)
        to = pl.ds(lane * BLK, BLK)

        @pl.when(from_mine)
        def _():
            out_ref[:, to, :] = mine_ref[:, pl.ds(start, BLK), :]

        @pl.when(jnp.logical_not(from_mine))
        def _():
            out_ref[:, to, :] = twin_ref[:, pl.ds(start, BLK), :]


def seat_kernel(rank_ref, ids, turn_ref, parts_ref, *refs, blocks_chip, side):
    is0 = lax.rem(rank_ref[0], 2) == 0
    for slot in range(ids.shape[0]):
        owner = owner_of(ids, slot, blocks_chip)
        source = jnp.where(is0, lax.rem(owner, side), lax.div(owner, side))
        turn = turn_of(ids, slot, blocks_chip)
        start = pl.multiple_of(lax.rem(turn, SEATS) * BLK, BLK)
        part = parts_ref[source, pl.ds(start, BLK), :]
        if len(refs) > 1:
            part = jnp.where(lax.div(turn, SEATS) == turn_ref[0], part, refs[0][slot])
        refs[-1][slot] = part


def gather_globals(mine, twin, global_ids, besides):
    devices = lax.axis_size("seq")
    side = math.isqrt(devices // 2)
    rank = lax.axis_index("seq")
    core, chip = rank % 2, rank // 2
    x, y = chip // side, chip % side
    heads, tok_rows, head_size = mine.shape
    slots = global_ids.shape[0]
    blocks_chip = 2 * (tok_rows // BLK)
    owner = global_ids // blocks_chip
    is0 = core == 0
    cross_pos = jnp.where(is0, x, y)
    owner_cross = jnp.where(is0, owner // side, owner % side)
    groups = [[(i * side + j) * 2 for j in range(side)] for i in range(side)]
    groups += [[(j * side + i) * 2 + 1 for j in range(side)] for i in range(side)]
    swap = [(i, i ^ 1) for i in range(devices)]
    scalars = [pl.BlockSpec(memory_space=pltpu.SMEM)] * 3
    vmem = pl.BlockSpec(memory_space=pltpu.VMEM)
    small = pltpu.CompilerParams(vmem_limit_bytes=16 << 20)

    def scatter(turn, held, run):
        spot = (rank.reshape(1), global_ids, turn.reshape(1))
        part, rounds = pl.pallas_call(
            pick_kernel,
            in_specs=[*scalars, vmem, vmem],
            out_specs=[vmem, scalars[0]],
            out_shape=[
                jax.ShapeDtypeStruct((heads, SEATS * BLK, head_size), mine.dtype),
                jax.ShapeDtypeStruct((1,), jnp.int32),
            ],
            compiler_params=small,
            name="pick",
        )(*spot, mine, twin)
        parts = lax.all_to_all(part, "seq", 0, 0, axis_index_groups=groups, tiled=True)
        (parts,) = run(part, (parts,))
        held = pl.pallas_call(
            lambda *refs: seat_kernel(*refs, blocks_chip=blocks_chip, side=side),
            in_specs=[*scalars, vmem, *[vmem] * len(held)],
            out_specs=vmem,
            out_shape=jax.ShapeDtypeStruct((slots, BLK, head_size), mine.dtype),
            compiler_params=small,
            name="seat",
        )(*spot, parts, *held)
        return held, rounds[0]

    held, last_turn = scatter(jnp.int32(0), [], besides[0])
    _, held = lax.while_loop(
        lambda carried: carried[0] > 0,
        lambda carried: (carried[0] - 1, scatter(carried[0], carried[1:], lambda _, parts: parts)[0]),
        (last_turn, held),
    )
    away = (owner_cross - cross_pos) % side
    before = held
    down, up = across_scatter(held, side, 3), across_scatter(held, side, -3)
    down, up = besides[1](before, (down, up))
    held = pick(away == side - 3, down, pick(away == 3, up, held))
    down, up = across_scatter(held, side, 1), across_scatter(held, side, -1)
    from_down = (away == side - 1) | (away == side // 2) | (away == 2)
    from_up = (away == 1) | (away == side - 2)
    held = pick(from_down, down, pick(from_up, up, held))
    before = held
    down, up = along_scatter(held, side, 3), along_scatter(held, side, -3)
    down, up = besides[2](before, (down, up))
    three = jnp.stack([held, down, up])
    before = three
    down, up = along_scatter(three, side, 1), along_scatter(three[:2], side, -1)
    down, up = besides[3](before, (down, up))
    own = jnp.concatenate([three, down, up]).reshape(heads, slots * BLK, head_size)
    (other,) = besides[4](own, (lax.ppermute(own, "seq", swap),))
    return own, other


def over_keys(one, two):
    return lax.dot_general(one, two, (((0,), (0,)), ((), ())), preferred_element_type=jnp.float32)


def over_head(one, two):
    return lax.dot_general(one, two, (((1,), (1,)), ((), ())), preferred_element_type=jnp.float32)


def window_kernel(rank_ref, low_ref, q_ref, near, mine, rest, *refs, scale):
    acc_ref, peak_ref, sum_ref = refs[-3:]
    group, tok_rows, head_size = q_ref.shape
    is0 = lax.rem(rank_ref[0], 2) == 0
    near_a, near_b, own_a, own_b = near[0, 0], near[1, 0], mine[0], rest[0]
    keys = [jnp.where(is0, near_b, near_a), jnp.where(is0, own_a, own_b)]
    vals = [jnp.where(is0, near_a, near_b), jnp.where(is0, own_b, own_a)]
    keys, vals = jnp.concatenate(keys, axis=0), jnp.concatenate(vals, axis=0)
    span = WIN * BLK
    rows = group * BLK
    for b in range(tok_rows // BLK):
        queries = q_ref[:, b * BLK : (b + 1) * BLK, :].reshape(rows, head_size)
        scores = over_head(keys[b * BLK : b * BLK + span], queries) * scale
        key_at = lax.broadcasted_iota(jnp.int32, (span, rows), 0) + b * BLK
        query_at = lax.broadcasted_iota(jnp.int32, (1, rows), 1) % BLK + (tok_rows + b * BLK)
        allowed = (key_at >= low_ref[b]) & (key_at <= query_at)
        scores = jnp.where(allowed, scores, masked_score)
        peak = jnp.max(scores, axis=0, keepdims=True)
        terms = jnp.exp2(scores - peak)
        sum_ref[0, b] = jnp.sum(terms, axis=0, keepdims=True)
        peak_ref[0, b] = peak
        acc_ref[0, b] = over_keys(vals[b * BLK : b * BLK + span], terms.astype(jnp.bfloat16))


def global_kernel(
    place, rank_ref, ids, q_ref, own_ref, other_ref, acc_ref, peak_ref, sum_ref, out_ref,
    *score_refs, scale,
):
    kv_count, blocks_here, head_size, rows = acc_ref.shape
    pair = score_refs[0].shape[0]
    side = place.shape[0]
    group = rows // BLK
    slots = ids.shape[0]
    rank = rank_ref[0]
    chip = lax.div(rank, 2)
    x, y = lax.div(chip, side), lax.rem(chip, side)
    is0 = lax.rem(rank, 2) == 0
    step = pl.program_id(0)

    def score(step, b):
        for j in range(pair):
            head = step * pair + j
            at = place[lax.rem(head - y + side, side)]
            keys = jnp.where(is0, own_ref[at], other_ref[at])
            queries = q_ref[pl.ds(head * group, group), b * BLK : (b + 1) * BLK, :]
            score_refs[b][j] = over_head(keys, queries.reshape(rows, head_size))

    def attend(step, b):
        gaps = [rank * blocks_here + b - ids[s] for s in range(slots)]
        bias = [jnp.where((g >= 0) & (g < WIN), masked_score, 0.0) for g in gaps]
        outs = []
        for j in range(pair):
            head = step * pair + j
            at = place[lax.rem(head - x + side, side)]
            vals = jnp.where(is0, other_ref[at], own_ref[at])
            before = peak_ref[head, b]
            peak = before
            for s in range(slots):
                top = jnp.max(score_refs[b][j, s * BLK : (s + 1) * BLK], axis=0, keepdims=True)
                peak = jnp.maximum(peak, top * scale + bias[s])
            factor = jnp.exp2(before - peak)
            total = sum_ref[head, b] * factor
            terms = []
            for s in range(slots):
                part = score_refs[b][j, s * BLK : (s + 1) * BLK]
                term = jnp.exp2(part * scale - (peak - bias[s]))
                total = total + jnp.sum(term, axis=0, keepdims=True)
                terms.append(term.astype(jnp.bfloat16))
            acc = acc_ref[head, b] * factor + over_keys(vals, jnp.concatenate(terms, axis=0))
            outs.append((acc * (1.0 / total)).T.reshape(group, BLK, head_size))
        rows_out = jnp.transpose(jnp.concatenate(outs, axis=0), (1, 0, 2))
        out_ref[b * BLK : (b + 1) * BLK] = rows_out.astype(out_ref.dtype)

    @pl.when(step == 0)
    def _():
        score(step, 0)

    for b in range(blocks_here):
        attend(step, b)
        if b + 1 < blocks_here:
            score(step, b + 1)
        else:
            score(jnp.minimum(step + 1, pl.num_programs(0) - 1), 0)


def per_device(queries, keys, values, global_ids, doc_lengths):
    tok_rows, heads_here, head_size = queries.shape
    kv_count = keys.shape[1]
    group = heads_here // kv_count
    blocks_here = tok_rows // BLK
    rows = group * BLK
    slots = global_ids.shape[0]
    scale = math.log2(math.e) / math.sqrt(head_size)
    rank = lax.axis_index("seq")
    devices = lax.axis_size("seq")
    side = math.isqrt(devices // 2)
    first_pos = rank * tok_rows
    doc_ends = jnp.cumsum(doc_lengths)
    query_pos = first_pos + jnp.arange(tok_rows, dtype=jnp.int32)
    is0 = rank % 2 == 0
    mine = jnp.where(is0, keys, values).transpose(1, 0, 2)
    rest = jnp.where(is0, values, keys).transpose(1, 0, 2)
    twin = lax.ppermute(rest, "seq", [(i, i ^ 1) for i in range(devices)])

    acc_shape = jax.ShapeDtypeStruct((kv_count, blocks_here, head_size, rows), jnp.float32)
    row_shape = jax.ShapeDtypeStruct((kv_count, blocks_here, 1, rows), jnp.float32)
    work = blocks_here * rows * BLK * WIN
    ring = [(i, i + 1) for i in range(devices - 1)]
    ready, state = {}, []

    def send_near(before, results):
        mine_now, rest_now, ends, _ = lax.optimization_barrier((mine, rest, doc_ends, before))
        begun = ends[None, :] <= query_pos[:, None]
        low = jnp.max(jnp.where(begun, ends[None, :], 0), axis=1) - (first_pos - tok_rows)
        low = jnp.tile(low.reshape(blocks_here, 1, BLK), (1, 1, group))
        near = lax.ppermute(jnp.stack([mine_now, rest_now]), "seq", ring)
        *results, low = lax.optimization_barrier((*results, low))
        ready.update(low=low, near=near)
        return results

    def lay_queries(before, results):
        given, _ = lax.optimization_barrier((queries, before))
        *results, by_head = lax.optimization_barrier((*results, given.transpose(1, 0, 2)))
        ready.update(by_head=by_head)
        return results

    def window_part(first, count, by_head):
        per_head = pl.BlockSpec((1, tok_rows, head_size), lambda k: (k + first, 0, 0))
        acc_spec = pl.BlockSpec((1, blocks_here, head_size, rows), lambda k: (k + first, 0, 0, 0))
        row_spec = pl.BlockSpec((1, blocks_here, 1, rows), lambda k: (k + first, 0, 0, 0))
        whole = [pl.BlockSpec(memory_space=pl.ANY)] * len(state)
        return pl.pallas_call(
            lambda *refs: window_kernel(*refs, scale=scale),
            grid=(count,),
            in_specs=[
                pl.BlockSpec(memory_space=pltpu.SMEM),
                pl.BlockSpec((blocks_here, 1, rows), lambda k: (0, 0, 0)),
                pl.BlockSpec((group, tok_rows, head_size), lambda k: (k + first, 0, 0)),
                pl.BlockSpec((2, 1, tok_rows, head_size), lambda k: (0, k + first, 0, 0)),
                per_head, per_head, *whole,
            ],
            out_specs=[acc_spec, row_spec, row_spec],
            out_shape=[acc_shape, row_shape, row_shape],
            input_output_aliases={6 + i: i for i in range(len(state))},
            cost_estimate=pl.CostEstimate(
                flops=4 * work * count * head_size,
                bytes_accessed=count << 20,
                transcendentals=work * count,
            ),
            compiler_params=pltpu.CompilerParams(vmem_limit_bytes=16 << 20),
            name=f"window_heads_{first}",
        )(rank.reshape(1), ready["low"], by_head, ready["near"], mine, rest, *state)

    def beside(first, count):
        def run(before, results):
            nonlocal state
            by_head, _ = lax.optimization_barrier((ready["by_head"], before))
            state = window_part(first, count, by_head)
            *results, acc, peak, total = lax.optimization_barrier((*results, *state))
            state = [acc, peak, total]
            return results

        return run

    quarter = kv_count // 4
    besides = [lay_queries, send_near, beside(0, 2 * quarter)]
    besides += [beside(2 * quarter, quarter), beside(3 * quarter, quarter)]
    own, other = gather_globals(mine, twin, global_ids, besides)
    place = [0] * side
    for at, offset in enumerate(HELD):
        place[offset % side] = at
    pair = 2
    whole = pl.BlockSpec(memory_space=pltpu.VMEM)
    return pl.pallas_call(
        lambda *refs: global_kernel(*refs, scale=scale),
        grid_spec=pltpu.PrefetchScalarGridSpec(
            num_scalar_prefetch=3,
            grid=(kv_count // pair,),
            in_specs=[whole] * 6,
            out_specs=pl.BlockSpec((tok_rows, pair * group, head_size), lambda k, *_: (0, k, 0)),
            scratch_shapes=[pltpu.VMEM((pair, slots * BLK, rows), jnp.float32)] * blocks_here,
        ),
        out_shape=jax.ShapeDtypeStruct((tok_rows, heads_here, head_size), jnp.bfloat16),
        compiler_params=pltpu.CompilerParams(vmem_limit_bytes=32 << 20),
        name="global_part",
    )(jnp.array(place, jnp.int32), rank.reshape(1), global_ids, ready["by_head"], own, other, *state)


def solution(mesh):
    shard = P(("grp", "seq"), None, None)
    return jax.shard_map(
        per_device,
        mesh=mesh,
        in_specs=(shard, shard, shard, P("grp"), P("grp")),
        out_specs=shard,
        check_vma=False,
    )
```

```python
import math

import jax
import jax.numpy as jnp
from jax import lax
from jax.experimental import pallas as pl
from jax.experimental.pallas import tpu as pltpu
from jax.sharding import PartitionSpec as P


BLK = 128
WIN = 3
masked_score = -1e30

HELD = (0, -3, 3, -1, -4, 2, 1, -2)

SEATS = 2


def ring_pairs(side, core0, core1):
    pairs = []
    for x in range(side):
        for y in range(side):
            for core, (dx, dy) in enumerate((core0, core1)):
                to = ((x + dx) % side) * side + (y + dy) % side
                pairs.append(((x * side + y) * 2 + core, to * 2 + core))
    return pairs


def along_scatter(shard, side, by):
    return lax.ppermute(shard, "seq", ring_pairs(side, (0, by), (by, 0)))


def across_scatter(shard, side, by):
    return lax.ppermute(shard, "seq", ring_pairs(side, (by, 0), (0, by)))


def pick(flag, one, other):
    return jnp.where(flag[:, None, None], one, other)


def owner_of(ids, slot, blocks_chip):
    return lax.div(ids[slot], blocks_chip)


def turn_of(ids, slot, blocks_chip):
    owner = owner_of(ids, slot, blocks_chip)
    return sum((owner_of(ids, s, blocks_chip) == owner).astype(jnp.int32) for s in range(slot))


def pick_kernel(rank_ref, ids, turn_ref, mine_ref, twin_ref, out_ref, rounds_ref):
    blocks_here = mine_ref.shape[1] // BLK
    blocks_chip = 2 * blocks_here
    chip, core = lax.div(rank_ref[0], 2), lax.rem(rank_ref[0], 2)
    last = jnp.int32(0)
    for slot in range(1, ids.shape[0]):
        last = jnp.maximum(last, turn_of(ids, slot, blocks_chip))
    rounds_ref[0] = lax.div(last, SEATS)
    for lane in range(SEATS):
        count, local = jnp.int32(0), jnp.int32(0)
        for slot in range(ids.shape[0]):
            on_chip = owner_of(ids, slot, blocks_chip) == chip
            hit = on_chip & (count == turn_ref[0] * SEATS + lane)
            local = jnp.where(hit, lax.rem(ids[slot], blocks_chip), local)
            count = count + on_chip.astype(jnp.int32)
        from_mine = lax.div(local, blocks_here) == core
        start = pl.multiple_of(lax.rem(local, blocks_here) * BLK, BLK)
        to = pl.ds(lane * BLK, BLK)

        @pl.when(from_mine)
        def _():
            out_ref[:, to, :] = mine_ref[:, pl.ds(start, BLK), :]

        @pl.when(jnp.logical_not(from_mine))
        def _():
            out_ref[:, to, :] = twin_ref[:, pl.ds(start, BLK), :]


def seat_kernel(rank_ref, ids, turn_ref, parts_ref, *refs, blocks_chip, side):
    is0 = lax.rem(rank_ref[0], 2) == 0
    for slot in range(ids.shape[0]):
        owner = owner_of(ids, slot, blocks_chip)
        source = jnp.where(is0, lax.rem(owner, side), lax.div(owner, side))
        turn = turn_of(ids, slot, blocks_chip)
        start = pl.multiple_of(lax.rem(turn, SEATS) * BLK, BLK)
        part = parts_ref[source, pl.ds(start, BLK), :]
        if len(refs) > 1:
            part = jnp.where(lax.div(turn, SEATS) == turn_ref[0], part, refs[0][slot])
        refs[-1][slot] = part


def gather_globals(mine, twin, global_ids, besides):
    devices = lax.axis_size("seq")
    side = math.isqrt(devices // 2)
    rank = lax.axis_index("seq")
    core, chip = rank % 2, rank // 2
    x, y = chip // side, chip % side
    heads, tok_rows, head_size = mine.shape
    slots = global_ids.shape[0]
    blocks_chip = 2 * (tok_rows // BLK)
    owner = global_ids // blocks_chip
    is0 = core == 0
    cross_pos = jnp.where(is0, x, y)
    owner_cross = jnp.where(is0, owner // side, owner % side)
    groups = [[(i * side + j) * 2 for j in range(side)] for i in range(side)]
    groups += [[(j * side + i) * 2 + 1 for j in range(side)] for i in range(side)]
    swap = [(i, i ^ 1) for i in range(devices)]
    scalars = [pl.BlockSpec(memory_space=pltpu.SMEM)] * 3
    vmem = pl.BlockSpec(memory_space=pltpu.VMEM)
    small = pltpu.CompilerParams(vmem_limit_bytes=16 << 20)

    def scatter(turn, held, run):
        spot = (rank.reshape(1), global_ids, turn.reshape(1))
        part, rounds = pl.pallas_call(
            pick_kernel,
            in_specs=[*scalars, vmem, vmem],
            out_specs=[vmem, scalars[0]],
            out_shape=[
                jax.ShapeDtypeStruct((heads, SEATS * BLK, head_size), mine.dtype),
                jax.ShapeDtypeStruct((1,), jnp.int32),
            ],
            compiler_params=small,
            name="pick",
        )(*spot, mine, twin)
        parts = lax.all_to_all(part, "seq", 0, 0, axis_index_groups=groups, tiled=True)
        parts = run(part, parts)
        held = pl.pallas_call(
            lambda *refs: seat_kernel(*refs, blocks_chip=blocks_chip, side=side),
            in_specs=[*scalars, vmem, *[vmem] * len(held)],
            out_specs=vmem,
            out_shape=jax.ShapeDtypeStruct((slots, BLK, head_size), mine.dtype),
            compiler_params=small,
            name="seat",
        )(*spot, parts, *held)
        return held, rounds[0]

    held, last_turn = scatter(jnp.int32(0), [], besides[0])
    _, held = lax.while_loop(
        lambda carried: carried[0] > 0,
        lambda carried: (carried[0] - 1, scatter(carried[0], carried[1:], lambda _, parts: parts)[0]),
        (last_turn, held),
    )
    away = (owner_cross - cross_pos) % side
    before = held
    down, up = across_scatter(held, side, 3), across_scatter(held, side, -3)
    down, up = besides[1](before, (down, up))
    held = pick(away == side - 3, down, pick(away == 3, up, held))
    before = held
    down, up = across_scatter(held, side, 1), across_scatter(held, side, -1)
    down, up = besides[2](before, (down, up))
    from_down = (away == side - 1) | (away == side // 2) | (away == 2)
    from_up = (away == 1) | (away == side - 2)
    held = pick(from_down, down, pick(from_up, up, held))
    before = held
    down, up = along_scatter(held, side, 3), along_scatter(held, side, -3)
    down, up = besides[3](before, (down, up))
    three = jnp.stack([held, down, up])
    before = three
    down, up = along_scatter(three, side, 1), along_scatter(three[:2], side, -1)
    down, up = besides[4](before, (down, up))
    own = jnp.concatenate([three, down, up]).reshape(heads, slots * BLK, head_size)
    other = lax.ppermute(own, "seq", swap)
    return own, other


def over_keys(one, two):
    return lax.dot_general(one, two, (((0,), (0,)), ((), ())), preferred_element_type=jnp.float32)


def over_head(one, two):
    return lax.dot_general(one, two, (((1,), (1,)), ((), ())), preferred_element_type=jnp.float32)


def window_kernel(rank_ref, low_ref, q_ref, near, mine, rest, *refs, scale):
    acc_ref, peak_ref, sum_ref = refs[-3:]
    group, tok_rows, head_size = q_ref.shape
    is0 = lax.rem(rank_ref[0], 2) == 0
    near_a, near_b, own_a, own_b = near[0, 0], near[1, 0], mine[0], rest[0]
    keys = [jnp.where(is0, near_b, near_a), jnp.where(is0, own_a, own_b)]
    vals = [jnp.where(is0, near_a, near_b), jnp.where(is0, own_b, own_a)]
    keys, vals = jnp.concatenate(keys, axis=0), jnp.concatenate(vals, axis=0)
    span = WIN * BLK
    rows = group * BLK
    for b in range(tok_rows // BLK):
        queries = q_ref[:, b * BLK : (b + 1) * BLK, :].reshape(rows, head_size)
        scores = over_head(keys[b * BLK : b * BLK + span], queries) * scale
        key_at = lax.broadcasted_iota(jnp.int32, (span, rows), 0) + b * BLK
        query_at = lax.broadcasted_iota(jnp.int32, (1, rows), 1) % BLK + (tok_rows + b * BLK)
        allowed = (key_at >= low_ref[b]) & (key_at <= query_at)
        scores = jnp.where(allowed, scores, masked_score)
        peak = jnp.max(scores, axis=0, keepdims=True)
        terms = jnp.exp2(scores - peak)
        sum_ref[0, b] = jnp.sum(terms, axis=0, keepdims=True)
        peak_ref[0, b] = peak
        acc_ref[0, b] = over_keys(vals[b * BLK : b * BLK + span], terms.astype(jnp.bfloat16))


def global_kernel(
    place, rank_ref, ids, q_ref, own_ref, other_ref, acc_ref, peak_ref, sum_ref, out_ref,
    *score_refs, scale,
):
    _, blocks_here, head_size, rows = acc_ref.shape
    pair = score_refs[0].shape[0]
    side = place.shape[0]
    group = rows // BLK
    slots = ids.shape[0]
    rank = rank_ref[0]
    chip = lax.div(rank, 2)
    x, y = lax.div(chip, side), lax.rem(chip, side)
    is0 = lax.rem(rank, 2) == 0
    step = pl.program_id(0)

    def score(step, b):
        for j in range(pair):
            head = step * pair + j
            at = place[lax.rem(head - y + side, side)]
            keys = jnp.where(is0, own_ref[at], other_ref[at])
            queries = q_ref[pl.ds(head * group, group), b * BLK : (b + 1) * BLK, :]
            score_refs[b][j] = over_head(keys, queries.reshape(rows, head_size))

    def attend(step, b):
        gaps = [rank * blocks_here + b - ids[s] for s in range(slots)]
        bias = [jnp.where((g >= 0) & (g < WIN), masked_score, 0.0) for g in gaps]
        outs = []
        for j in range(pair):
            head = step * pair + j
            at = place[lax.rem(head - x + side, side)]
            vals = jnp.where(is0, other_ref[at], own_ref[at])
            before = peak_ref[head, b]
            peak = before
            for s in range(slots):
                top = jnp.max(score_refs[b][j, s * BLK : (s + 1) * BLK], axis=0, keepdims=True)
                peak = jnp.maximum(peak, top * scale + bias[s])
            factor = jnp.exp2(before - peak)
            total = sum_ref[head, b] * factor
            terms = []
            for s in range(slots):
                part = score_refs[b][j, s * BLK : (s + 1) * BLK]
                term = jnp.exp2(part * scale - (peak - bias[s]))
                total = total + jnp.sum(term, axis=0, keepdims=True)
                terms.append(term.astype(jnp.bfloat16))
            acc = acc_ref[head, b] * factor + over_keys(vals, jnp.concatenate(terms, axis=0))
            outs.append((acc * (1.0 / total)).T.reshape(group, BLK, head_size))
        rows_out = jnp.transpose(jnp.concatenate(outs, axis=0), (1, 0, 2))
        out_ref[b * BLK : (b + 1) * BLK] = rows_out.astype(out_ref.dtype)

    @pl.when(step == 0)
    def _():
        score(step, 0)

    for b in range(blocks_here):
        attend(step, b)
        if b + 1 < blocks_here:
            score(step, b + 1)
        else:
            score(jnp.minimum(step + 1, pl.num_programs(0) - 1), 0)


def per_device(queries, keys, values, global_ids, doc_lengths):
    tok_rows, heads_here, head_size = queries.shape
    kv_count = keys.shape[1]
    group = heads_here // kv_count
    blocks_here = tok_rows // BLK
    rows = group * BLK
    slots = global_ids.shape[0]
    scale = math.log2(math.e) / math.sqrt(head_size)
    rank = lax.axis_index("seq")
    devices = lax.axis_size("seq")
    side = math.isqrt(devices // 2)
    first_pos = rank * tok_rows
    doc_ends = jnp.cumsum(doc_lengths)
    query_pos = first_pos + jnp.arange(tok_rows, dtype=jnp.int32)
    is0 = rank % 2 == 0
    mine = jnp.where(is0, keys, values).transpose(1, 0, 2)
    rest = jnp.where(is0, values, keys).transpose(1, 0, 2)
    twin = lax.ppermute(rest, "seq", [(i, i ^ 1) for i in range(devices)])

    acc_shape = jax.ShapeDtypeStruct((kv_count, blocks_here, head_size, rows), jnp.float32)
    row_shape = jax.ShapeDtypeStruct((kv_count, blocks_here, 1, rows), jnp.float32)
    work = blocks_here * rows * BLK * WIN
    ring = [(i, i + 1) for i in range(devices - 1)]
    ready, state = {}, []

    near = lax.ppermute(jnp.stack([mine, rest]), "seq", ring)

    def find_low(before, result):
        ends, _ = lax.optimization_barrier((doc_ends, before))
        begun = ends[None, :] <= query_pos[:, None]
        low = jnp.max(jnp.where(begun, ends[None, :], 0), axis=1) - (first_pos - tok_rows)
        low = jnp.tile(low.reshape(blocks_here, 1, BLK), (1, 1, group))
        result, low = lax.optimization_barrier((result, low))
        ready.update(low=low, near=near)
        return result

    def lay_queries(before, results):
        given, _ = lax.optimization_barrier((queries, before))
        *results, by_head = lax.optimization_barrier((*results, given.transpose(1, 0, 2)))
        ready.update(by_head=by_head)
        return results

    def window_part(first, count, by_head):
        per_head = pl.BlockSpec((1, tok_rows, head_size), lambda k: (k + first, 0, 0))
        acc_spec = pl.BlockSpec((1, blocks_here, head_size, rows), lambda k: (k + first, 0, 0, 0))
        row_spec = pl.BlockSpec((1, blocks_here, 1, rows), lambda k: (k + first, 0, 0, 0))
        whole = [pl.BlockSpec(memory_space=pl.ANY)] * len(state)
        return pl.pallas_call(
            lambda *refs: window_kernel(*refs, scale=scale),
            grid=(count,),
            in_specs=[
                pl.BlockSpec(memory_space=pltpu.SMEM),
                pl.BlockSpec((blocks_here, 1, rows), lambda k: (0, 0, 0)),
                pl.BlockSpec((group, tok_rows, head_size), lambda k: (k + first, 0, 0)),
                pl.BlockSpec((2, 1, tok_rows, head_size), lambda k: (0, k + first, 0, 0)),
                per_head, per_head, *whole,
            ],
            out_specs=[acc_spec, row_spec, row_spec],
            out_shape=[acc_shape, row_shape, row_shape],
            input_output_aliases={6 + i: i for i in range(len(state))},
            cost_estimate=pl.CostEstimate(
                flops=4 * work * count * head_size,
                bytes_accessed=count << 20,
                transcendentals=work * count,
            ),
            compiler_params=pltpu.CompilerParams(vmem_limit_bytes=16 << 20),
        )(rank.reshape(1), ready["low"], by_head, ready["near"], mine, rest, *state)

    def beside(first, count):
        def run(before, results):
            nonlocal state
            by_head, _ = lax.optimization_barrier((ready["by_head"], before))
            state = window_part(first, count, by_head)
            *results, acc, peak, total = lax.optimization_barrier((*results, *state))
            state = [acc, peak, total]
            return results

        return run

    quarter = kv_count // 4
    besides = [find_low, lay_queries, beside(0, quarter), beside(quarter, 2 * quarter)]
    besides.append(beside(3 * quarter, quarter))
    own, other = gather_globals(mine, twin, global_ids, besides)
    place = [0] * side
    for at, offset in enumerate(HELD):
        place[offset % side] = at
    pair = 2
    whole = pl.BlockSpec(memory_space=pltpu.VMEM)
    return pl.pallas_call(
        lambda *refs: global_kernel(*refs, scale=scale),
        grid_spec=pltpu.PrefetchScalarGridSpec(
            num_scalar_prefetch=3,
            grid=(kv_count // pair,),
            in_specs=[whole] * 6,
            out_specs=pl.BlockSpec((tok_rows, pair * group, head_size), lambda k, *_: (0, k, 0)),
            scratch_shapes=[pltpu.VMEM((pair, slots * BLK, rows), jnp.float32)] * blocks_here,
        ),
        out_shape=jax.ShapeDtypeStruct((tok_rows, heads_here, head_size), jnp.bfloat16),
        compiler_params=pltpu.CompilerParams(vmem_limit_bytes=32 << 20),
        name="global_part",
    )(jnp.array(place, jnp.int32), rank.reshape(1), global_ids, ready["by_head"], own, other, *state)


def solution(mesh):
    shard = P(("grp", "seq"), None, None)
    return jax.shard_map(
        per_device,
        mesh=mesh,
        in_specs=(shard, shard, shard, P("grp"), P("grp")),
        out_specs=shard,
        check_vma=False,
    )
```
